128 devices in a mesh: band: 64 (over y, z, x_hi, core), grid: 2 (over x_lo).
Axes of the slice: x: 4 (x_hi: 2, x_lo: 2; x = x_hi * 2 + x_lo), y: 4, z: 4, core: 2. Of those that a mesh axis runs over, the one named last changes fastest.
Arguments:
- bands: float32 [128, 72, 5184], P('band', 'grid'), may hold values from -2.4 to 2.4
Outputs:
- exchange_terms: float32 [128, 72, 5184], P('band', 'grid')
The draws below stay inside these ranges and needn't reach their ends.
All inputs are finite; a program needn't handle non-finite values.
Results may differ from the reference program's by a relative error of at most 0.0001.
Values sent between devices are 32-bit elements; how exact they have to be, the bound alone decides.
A program may use at most 128 MiB of HBM per device.

```python
import math
import jax
import jax.numpy as jnp
from jax import lax

GRID = 72
BAND_DEV = 2
STEPS = 3
BLOCKS = 64
BANDS = 128


def draw_bands(key, part):
    shape = (BANDS, GRID, GRID * GRID)
    return 0.4 * jax.random.truncated_normal(key, -6.0, 6.0, shape, jnp.float32)


def setup_inputs(seed: int = 0) -> dict:
    keys = jax.random.split(jax.random.key(seed), 2)
    return {
        "bands": draw_bands(jax.random.fold_in(keys[1], 71), 0),
    }


spacing = 0.5167


def tables(count):
    index = jnp.arange(count, dtype=jnp.int32)
    half = count // 2
    freq = jnp.where(index <= half, index, index - half)
    phase = ((freq[:, None] * index[None, :]) % count).astype(jnp.float32) * (2.0 * math.pi / count)
    table = jnp.where(index[:, None] <= half, jnp.cos(phase), jnp.sin(phase))
    weight = jnp.where((index == 0) | (index == half), 1.0, 2.0).astype(jnp.float32)
    square = freq.astype(jnp.float32) ** 2
    factor = (2.0 * math.pi / (count * spacing)) ** 2
    ksq = factor * (square[:, None, None] + square[None, :, None] + square[None, None, :])
    safe = jnp.where(ksq > 0, ksq, 1.0)
    coulomb = jnp.where(ksq > 0, 4.0 * math.pi / safe, 0.0)
    weights = weight[:, None, None] * weight[None, :, None] * weight[None, None, :]
    kernel = (coulomb * weights / float(count ** 3)).astype(jnp.float32)
    return table, kernel.reshape(count, count * count)


def forward_axis(values, table):
    return jnp.einsum('pmc,kc->pkm', values, table, precision=lax.Precision.HIGHEST)


def inverse_axis(values, table):
    return jnp.einsum('pmk,kr->prm', values, table, precision=lax.Precision.HIGHEST)


def coulomb_filter(density, table, kernel):
    count = table.shape[0]
    pairs = density.shape[0]
    work = forward_axis(density.reshape(pairs, count * count, count), table)
    work = forward_axis(work.reshape(pairs, count * count, count), table)
    work = forward_axis(work.reshape(pairs, count * count, count), table)
    work = work * kernel[None]
    work = inverse_axis(work.reshape(pairs, count * count, count), table)
    work = inverse_axis(work.reshape(pairs, count * count, count), table)
    work = inverse_axis(work.reshape(pairs, count * count, count), table)
    return work


def pair_terms(home, visit, table, kernel):
    home_count = home.shape[0]
    visit_count = visit.shape[0]
    count = home.shape[1]
    density = (home[:, None] * visit[None]).reshape(home_count * visit_count, count, home.shape[2])
    potential = coulomb_filter(density, table, kernel).reshape(home_count, visit_count, count, home.shape[2])
    home_part = -jnp.sum(potential * visit[None], axis=1)
    partner = -jnp.sum(potential * home[:, None], axis=0)
    return home_part, partner


def reference(bands):
    table, kernel = tables(GRID)
    blocks = bands.reshape(BLOCKS, BAND_DEV, GRID, GRID * GRID)
    total = jnp.zeros_like(blocks)
    for step in range(1, STEPS + 1):
        visiting = jnp.roll(blocks, step, axis=0)

        def one_block(pair):
            return pair_terms(pair[0], pair[1], table, kernel)

        home_part, partner = lax.map(one_block, (blocks, visiting))
        total = total + home_part + jnp.roll(partner, -step, axis=0)
    return total.reshape(bands.shape)
```

```python
import functools
import math

import jax
import jax.numpy as jnp
import numpy as np
from jax import lax
from jax.experimental import pallas as pl
from jax.experimental.pallas import tpu as pltpu
from jax.sharding import PartitionSpec as P

N = 72
HALF = 36
LANES = 128
ROWS = N * N
PLANE = N * N
STEPS = 3
STRIP = 8
spacing = 0.5167


def shifted(value, axis, steps):
    count = lax.axis_size(axis)
    pairs = [(source, (source + steps) % count) for source in range(count)]
    return lax.ppermute(value, axis, pairs)


def split_up(array, dim, devices):
    before, after = (array.shape[:dim], array.shape[dim + 1 :])
    return jnp.moveaxis(array.reshape(*before, devices, -1, *after), dim, 0)


def sent_and_summed(array, axis, dim):
    devices = lax.axis_size(axis)
    blocks = lax.all_to_all(split_up(array, dim, devices), axis, 0, 0, tiled=True)
    return jnp.sum(blocks, axis=0)


def rounded(x):
    return x.astype(jnp.bfloat16).astype(np.float32)


def constants():
    index = np.arange(N)
    freq = np.where(index <= HALF, index, index - HALF)
    phase = (freq[:, None] * index[None, :] % N) * (2.0 * math.pi / N)
    table = np.where(index[:, None] <= HALF, np.cos(phase), np.sin(phase)).astype(np.float32)

    def stacked(t):
        return np.concatenate([t, t, t - rounded(t)], axis=1)

    def blocks(m):
        wide = np.zeros((2 * N, 2 * LANES), np.float32)
        wide[:N, :N] = m
        wide[N:, LANES : LANES + N] = m
        return np.stack([rounded(wide), rounded(wide - rounded(wide))])

    return stacked(table), stacked(table.T), blocks(table.T), blocks(table.T).transpose(0, 2, 1)


def dot(a, b):
    return jnp.dot(a, b, preferred_element_type=jnp.float32, precision=lax.Precision.DEFAULT)


def low_part(x):
    return x - x.astype(jnp.bfloat16).astype(jnp.float32)


def down(table, x):
    return dot(table, jnp.concatenate([x, low_part(x), x], axis=0))


def along(x, high, low):
    return dot(x, high) + dot(low_part(x), high) + dot(x, low)


def fill_tables(wide_ahead, wide_back, lane_ahead, lane_back, factors):
    rows = lax.broadcasted_iota(jnp.int32, (2 * N, 2 * LANES), 0)
    cols = lax.broadcasted_iota(jnp.int32, (2 * N, 2 * LANES), 1)
    for u in range(8):
        start = 2 * N * u % LANES
        move = jnp.where(cols == rows + start, 1.0, 0.0)
        for part in range(2):
            lane_ahead[u, part] = jnp.zeros((2 * LANES, 2 * LANES), jnp.float32)
            lane_ahead[u, part, start : start + 2 * N, :] = wide_ahead[part]
            lane_back[u, part] = dot(wide_back[part], move)

    def wave(i):
        f = jnp.where(i <= HALF, i, i - HALF)
        return (f * f).astype(jnp.float32), jnp.where((i == 0) | (i == HALF), 1.0, 2.0).astype(jnp.float32)

    factor = (2.0 * math.pi / (N * spacing)) ** 2
    square_b, weight_b = wave(lax.broadcasted_iota(jnp.int32, (N, LANES), 0))
    square_c, weight_c = wave(lax.broadcasted_iota(jnp.int32, (N, LANES), 1))
    inside = lax.broadcasted_iota(jnp.int32, (N, LANES), 1) < N

    def fill(i, _):
        square_a, weight_a = wave(i)
        ksq = factor * (square_a + square_b + square_c)
        keep = (ksq > 0) & inside
        coulomb = jnp.where(keep, 4.0 * math.pi / jnp.where(keep, ksq, 1.0), 0.0)
        factors[pl.ds(pl.multiple_of(i * N, 8), N), :] = coulomb * (weight_a * weight_b * weight_c) / float(N**3)
        return 0

    lax.fori_loop(0, N, fill, 0)


def exchange(homes, visit, home_outs, visit_out, first, ahead, back, lane_ahead, lane_back, factors, u, w):
    BODY = 5
    WIDE = 2 * LANES
    TAIL = PLANE // WIDE * WIDE

    def flat_ahead(tiles):
        for at, width in tiles:
            for p in range(2):
                x = homes[p][:, pl.ds(at, width)] * visit[:, pl.ds(at, width)]
                if width < LANES:
                    x = jnp.concatenate([x, jnp.zeros((N, LANES - width), jnp.float32)], axis=1)
                u[p, :, pl.ds(at, max(width, LANES))] = down(ahead[...], x)

    def wide_tiles(i):
        return [(pl.multiple_of((i * BODY + k) * WIDE, LANES), WIDE) for k in range(BODY)]

    def pass_1(i, _):
        flat_ahead(wide_tiles(i))
        return 0

    lax.fori_loop(0, TAIL // WIDE // BODY, pass_1, 0)
    flat_ahead([(TAIL, PLANE - TAIL)])

    def lines_ahead(t, count):
        base = pl.multiple_of(t * 9 * LANES, LANES)
        for k in range(count):
            at = 2 * N * k // LANES * LANES
            x = jnp.concatenate([u[p, :, pl.ds(base + at, WIDE)] for p in range(2)], axis=0)
            y = along(x, lane_ahead[k, 0], lane_ahead[k, 1])
            r = pl.multiple_of((t * 8 + k) * 2 * N, 8)
            for p in range(2):
                w[p, pl.ds(r, N), :] = y[N * p : N * (p + 1), :LANES]
                w[p, pl.ds(r + N, N), :] = y[N * p : N * (p + 1), LANES:]

    def pass_2(t, _):
        lines_ahead(t, 8)
        return 0

    lax.fori_loop(0, 4, pass_2, 0)
    lines_ahead(4, 4)

    def load_w(i):
        rows = pl.ds(i, N, stride=N)
        return jnp.concatenate([w[0, rows, :], w[1, rows, :]], axis=1)

    def store_w(i, y):
        rows = pl.ds(i, N, stride=N)
        w[0, rows, :] = y[:, :LANES]
        w[1, rows, :] = y[:, LANES:]

    def ahead_b(i, x):
        y = down(ahead[...], x)
        f = factors[pl.ds(pl.multiple_of(i * N, 8), N), :]
        return y * jnp.concatenate([f, f], axis=1)

    def pass_3(i, _):
        now = [i * STRIP + k for k in range(STRIP)]
        before = [i * STRIP - STRIP + k for k in range(STRIP)]
        xs, ys = [load_w(q) for q in now], [load_w(q) for q in before]
        xs = [ahead_b(q, x) for q, x in zip(now, xs)]
        ys = [down(back[...], y) for y in ys]
        for q, x in zip(now, xs):
            store_w(q, x)
        for q, y in zip(before, ys):
            store_w(q, y)
        return 0

    for q, x in [(q, ahead_b(q, load_w(q))) for q in range(STRIP)]:
        store_w(q, x)
    lax.fori_loop(1, N // STRIP, pass_3, 0)
    for q, y in [(q, down(back[...], load_w(q))) for q in range(N - STRIP, N)]:
        store_w(q, y)

    def lines_back(t, count):
        base = pl.multiple_of(t * 9 * LANES, LANES)
        total = {}
        for k in range(count):
            tile = 2 * N * k // LANES
            r = pl.multiple_of((t * 8 + k) * 2 * N, 8)
            x = jnp.concatenate(
                [jnp.concatenate([w[p, pl.ds(r, N), :], w[p, pl.ds(r + N, N), :]], axis=1) for p in range(2)], axis=0
            )
            y = along(x, lane_back[k, 0], lane_back[k, 1])
            for half in range(2):
                part = y[:, LANES * half : LANES * (half + 1)]
                total[tile + half] = total[tile + half] + part if tile + half in total else part
        for tile, value in total.items():
            for p in range(2):
                u[p, :, pl.ds(base + tile * LANES, LANES)] = value[N * p : N * (p + 1)]

    def pass_4(t, _):
        lines_back(t, 8)
        return 0

    lax.fori_loop(0, 4, pass_4, 0)
    lines_back(4, 4)

    def flat_back(tiles):
        for at, width in tiles:
            cells = pl.ds(at, width)
            total = None
            for p in range(2):
                v = down(back[...], u[p, :, pl.ds(at, max(width, LANES))])[:, :width]
                mine = v * visit[:, cells]
                home_outs[p][:, cells] = -mine if first else home_outs[p][:, cells] - mine
                part = v * homes[p][:, cells]
                total = part if total is None else total + part
            visit_out[:, cells] = -total

    def pass_5(i, _):
        flat_back(wide_tiles(i))
        return 0

    lax.fori_loop(0, TAIL // WIDE // BODY, pass_5, 0)
    flat_back([(TAIL, PLANE - TAIL)])


def kernel(
    home_in, visit_in, ahead, back, wide_ahead, wide_back, home_out, visit_out,
    flat, outs, lane_ahead, lane_back, factors, u, w, sems,
):
    copies = [pltpu.make_async_copy(home_in.at[i], flat.at[i], sems.at[i]) for i in range(2)]
    copies += [pltpu.make_async_copy(visit_in.at[i], flat.at[2 + i], sems.at[2 + i]) for i in range(3)]
    for copy in copies:
        copy.start()
    fill_tables(wide_ahead, wide_back, lane_ahead, lane_back, factors)
    for copy in copies:
        copy.wait()
    for j in range(3):
        exchange(
            [flat.at[0], flat.at[1]], flat.at[2 + j], [outs.at[0], outs.at[1]], outs.at[2 + j], j == 0,
            ahead, back, lane_ahead, lane_back, factors, u, w,
        )
    copies = [pltpu.make_async_copy(outs.at[i], home_out.at[i], sems.at[i]) for i in range(2)]
    copies += [pltpu.make_async_copy(outs.at[2 + i], visit_out.at[i], sems.at[2 + i]) for i in range(3)]
    for copy in copies:
        copy.start()
    for copy in copies:
        copy.wait()


def pair_terms(home, visit, consts):
    hbm = pl.BlockSpec(memory_space=pl.ANY)
    vmem = pl.BlockSpec(memory_space=pltpu.VMEM)
    return pl.pallas_call(
        kernel,
        out_shape=(
            jax.ShapeDtypeStruct((2, N, PLANE), jnp.float32),
            jax.ShapeDtypeStruct((3, N, PLANE), jnp.float32),
        ),
        in_specs=[hbm, hbm, vmem, vmem, vmem, vmem],
        out_specs=(hbm, hbm),
        scratch_shapes=[
            pltpu.VMEM((5, N, PLANE), jnp.float32),
            pltpu.VMEM((5, N, PLANE), jnp.float32),
            pltpu.VMEM((8, 2, 2 * LANES, 2 * LANES), jnp.float32),
            pltpu.VMEM((8, 2, 2 * LANES, 2 * LANES), jnp.float32),
            pltpu.VMEM((ROWS, LANES), jnp.float32),
            pltpu.VMEM((2, N, 41 * LANES), jnp.float32),
            pltpu.VMEM((2, ROWS, LANES), jnp.float32),
            pltpu.SemaphoreType.DMA((5,)),
        ],
        compiler_params=pltpu.CompilerParams(vmem_limit_bytes=60 * 1024 * 1024),
        name="pair_terms",
    )(home, visit, *consts)


def local(bands):
    consts = constants()
    whole = lax.all_gather(bands, "grid", axis=1, tiled=True)
    share = whole.shape[0] // lax.axis_size("grid")
    first = lax.axis_index("grid") * share
    visit = lax.dynamic_slice_in_dim(whole, first, share, 0)
    visits = jnp.concatenate([shifted(visit, "band", s) for s in (1, 2, 3)], axis=0)
    home_total, parts = pair_terms(whole, visits, consts)
    carried = sum(shifted(parts[s : s + 1], "band", -(s + 1)) for s in range(3))
    own_rows = lax.dynamic_slice_in_dim(home_total, first, share, 0) + carried
    home_total = lax.dynamic_update_slice_in_dim(home_total, own_rows, first, 0)
    return sent_and_summed(home_total, "grid", 1)


def solution(mesh):
    return jax.shard_map(
        local,
        mesh=mesh,
        in_specs=(P("band", "grid", None),),
        out_specs=P("band", "grid", None),
        check_vma=False,
    )
```

```python
import functools
import math

import jax
import jax.numpy as jnp
import numpy as np
from jax import lax
from jax.experimental import pallas as pl
from jax.experimental.pallas import tpu as pltpu
from jax.sharding import PartitionSpec as P

N = 72
HALF = 36
LANES = 128
ROWS = N * N
PLANE = N * N
MESH = pl.DeviceIdType.MESH
PADDED = 80
CHUNKS = ((0, 1792), (1792, 1792), (3584, 1600))
STRIP = 8
spacing = 0.5167


def rounded(x):
    return x.astype(jnp.bfloat16).astype(np.float32)


def constants():
    index = np.arange(N)
    freq = np.where(index <= HALF, index, index - HALF)
    phase = (freq[:, None] * index[None, :] % N) * (2.0 * math.pi / N)
    table = np.where(index[:, None] <= HALF, np.cos(phase), np.sin(phase)).astype(np.float32)

    def stacked(t):
        return np.concatenate([t, t, t - rounded(t)], axis=1)

    def blocks(m):
        wide = np.zeros((2 * N, 2 * LANES), np.float32)
        wide[:N, :N] = m
        wide[N:, LANES : LANES + N] = m
        return np.stack([rounded(wide), rounded(wide - rounded(wide))])

    halves = np.concatenate([np.arange(HALF), np.arange(HALF) + PADDED // 2])
    halved = np.zeros((N, PADDED), np.float32)
    halved[:, halves] = table
    return stacked(table), stacked(table.T), stacked(halved), stacked(halved.T), blocks(table.T), blocks(table.T).transpose(0, 2, 1)


def dot(a, b):
    return jnp.dot(a, b, preferred_element_type=jnp.float32, precision=lax.Precision.DEFAULT)


def low_part(x):
    return x - x.astype(jnp.bfloat16).astype(jnp.float32)


def down(table, x):
    return dot(table, jnp.concatenate([x, low_part(x), x], axis=0))


def joined(x):
    gap = jnp.zeros((PADDED // 2 - HALF, x[0].shape[1]), jnp.float32)
    return jnp.concatenate([x[0], gap, x[1], gap], axis=0)


def along(x, high, low):
    return dot(x, high) + dot(low_part(x), high) + dot(x, low)


def fill_tables(wide_ahead, wide_back, lane_ahead, lane_back, factors):
    rows = lax.broadcasted_iota(jnp.int32, (2 * N, 2 * LANES), 0)
    cols = lax.broadcasted_iota(jnp.int32, (2 * N, 2 * LANES), 1)
    for u in range(8):
        start = 2 * N * u % LANES
        move = jnp.where(cols == rows + start, 1.0, 0.0)
        for part in range(2):
            lane_ahead[u, part] = jnp.zeros((2 * LANES, 2 * LANES), jnp.float32)
            lane_ahead[u, part, start : start + 2 * N, :] = wide_ahead[part]
            lane_back[u, part] = dot(wide_back[part], move)

    def wave(i):
        f = jnp.where(i <= HALF, i, i - HALF)
        return (f * f).astype(jnp.float32), jnp.where((i == 0) | (i == HALF), 1.0, 2.0).astype(jnp.float32)

    factor = (2.0 * math.pi / (N * spacing)) ** 2
    square_b, weight_b = wave(lax.broadcasted_iota(jnp.int32, (N, LANES), 0))
    square_c, weight_c = wave(lax.broadcasted_iota(jnp.int32, (N, LANES), 1))
    inside = lax.broadcasted_iota(jnp.int32, (N, LANES), 1) < N

    def fill(i, _):
        square_a, weight_a = wave(i)
        ksq = factor * (square_a + square_b + square_c)
        keep = (ksq > 0) & inside
        coulomb = jnp.where(keep, 4.0 * math.pi / jnp.where(keep, ksq, 1.0), 0.0)
        factors[pl.ds(pl.multiple_of(i * N, 8), N), :] = coulomb * (weight_a * weight_b * weight_c) / float(N**3)
        return 0

    lax.fori_loop(0, N, fill, 0)


def exchange(homes, visit, home_outs, visit_out, first, tables, lane_ahead, lane_back, factors, u, w):
    ahead, back, half_ahead, half_back = tables
    BODY = 5
    WIDE = 2 * LANES
    TAIL = PLANE // WIDE * WIDE

    def flat_ahead(tiles):
        for at, width in tiles:
            for p in range(2):
                x = joined([homes[p][h, :, pl.ds(at, width)] * visit[h, :, pl.ds(at, width)] for h in range(2)])
                if width < LANES:
                    x = jnp.concatenate([x, jnp.zeros((PADDED, LANES - width), jnp.float32)], axis=1)
                u[p, :, pl.ds(at, max(width, LANES))] = down(half_ahead[...], x)

    def wide_tiles(i):
        return [(pl.multiple_of((i * BODY + k) * WIDE, LANES), WIDE) for k in range(BODY)]

    def pass_1(i, _):
        flat_ahead(wide_tiles(i))
        return 0

    lax.fori_loop(0, TAIL // WIDE // BODY, pass_1, 0)
    flat_ahead([(TAIL, PLANE - TAIL)])

    def lines_ahead(t, count):
        base = pl.multiple_of(t * 9 * LANES, LANES)
        for k in range(count):
            at = 2 * N * k // LANES * LANES
            x = jnp.concatenate([u[p, :, pl.ds(base + at, WIDE)] for p in range(2)], axis=0)
            y = along(x, lane_ahead[k, 0], lane_ahead[k, 1])
            r = pl.multiple_of((t * 8 + k) * 2 * N, 8)
            for p in range(2):
                w[p, pl.ds(r, N), :] = y[N * p : N * (p + 1), :LANES]
                w[p, pl.ds(r + N, N), :] = y[N * p : N * (p + 1), LANES:]

    def pass_2(t, _):
        lines_ahead(t, 8)
        return 0

    lax.fori_loop(0, 4, pass_2, 0)
    lines_ahead(4, 4)

    def load_w(i):
        rows = pl.ds(i, N, stride=N)
        return jnp.concatenate([w[0, rows, :], w[1, rows, :]], axis=1)

    def store_w(i, y):
        rows = pl.ds(i, N, stride=N)
        w[0, rows, :] = y[:, :LANES]
        w[1, rows, :] = y[:, LANES:]

    def ahead_b(i, x):
        y = down(ahead[...], x)
        f = factors[pl.ds(pl.multiple_of(i * N, 8), N), :]
        return y * jnp.concatenate([f, f], axis=1)

    def pass_3(i, _):
        now = [i * STRIP + k for k in range(STRIP)]
        before = [i * STRIP - STRIP + k for k in range(STRIP)]
        xs, ys = [load_w(q) for q in now], [load_w(q) for q in before]
        xs = [ahead_b(q, x) for q, x in zip(now, xs)]
        ys = [down(back[...], y) for y in ys]
        for q, x in zip(now, xs):
            store_w(q, x)
        for q, y in zip(before, ys):
            store_w(q, y)
        return 0

    for q, x in [(q, ahead_b(q, load_w(q))) for q in range(STRIP)]:
        store_w(q, x)
    lax.fori_loop(1, N // STRIP, pass_3, 0)
    for q, y in [(q, down(back[...], load_w(q))) for q in range(N - STRIP, N)]:
        store_w(q, y)

    def lines_back(t, count):
        base = pl.multiple_of(t * 9 * LANES, LANES)
        total = {}
        for k in range(count):
            tile = 2 * N * k // LANES
            r = pl.multiple_of((t * 8 + k) * 2 * N, 8)
            x = jnp.concatenate(
                [jnp.concatenate([w[p, pl.ds(r, N), :], w[p, pl.ds(r + N, N), :]], axis=1) for p in range(2)], axis=0
            )
            y = along(x, lane_back[k, 0], lane_back[k, 1])
            for half in range(2):
                part = y[:, LANES * half : LANES * (half + 1)]
                total[tile + half] = total[tile + half] + part if tile + half in total else part
        for tile, value in total.items():
            for p in range(2):
                u[p, :, pl.ds(base + tile * LANES, LANES)] = value[N * p : N * (p + 1)]

    def pass_4(t, _):
        lines_back(t, 8)
        return 0

    lax.fori_loop(0, 4, pass_4, 0)
    lines_back(4, 4)

    def flat_back(tiles):
        for at, width in tiles:
            cells = pl.ds(at, width)
            total = [0.0, 0.0]
            for p in range(2):
                v = down(half_back[...], u[p, :, pl.ds(at, max(width, LANES))])[:, :width]
                for h in range(2):
                    part = v[PADDED // 2 * h : PADDED // 2 * h + HALF]
                    mine = part * visit[h, :, cells]
                    home_outs[p][h, :, cells] = -mine if first else home_outs[p][h, :, cells] - mine
                    total[h] = total[h] - part * homes[p][h, :, cells]
            for h in range(2):
                visit_out[h, :, cells] = total[h]

    def pass_5(i, _):
        flat_back(wide_tiles(i))
        return 0

    lax.fori_loop(0, TAIL // WIDE // BODY, pass_5, 0)
    flat_back([(TAIL, PLANE - TAIL)])


def pair_kernel(
    own, other, visit_in, ahead, back, half_ahead, half_back, wide_ahead, wide_back, home_out, visit_out,
    flat, outs, lane_ahead, lane_back, factors, u, w, sems,
):
    g = lax.axis_index("grid")
    copies = [pltpu.make_async_copy(own.at[b], flat.at[b, g], sems.at[b]) for b in range(2)]
    copies += [pltpu.make_async_copy(other.at[b], flat.at[b, 1 - g], sems.at[2 + b]) for b in range(2)]
    copies += [pltpu.make_async_copy(visit_in.at[i], flat.at[2 + i], sems.at[4 + i]) for i in range(3)]
    for copy in copies:
        copy.start()
    fill_tables(wide_ahead, wide_back, lane_ahead, lane_back, factors)
    for copy in copies:
        copy.wait()
    outgoing = []
    for j in range(3):
        exchange(
            [flat.at[0], flat.at[1]], flat.at[2 + j], [outs.at[0], outs.at[1]], outs.at[2 + j], j == 0,
            (ahead, back, half_ahead, half_back), lane_ahead, lane_back, factors, u, w,
        )
        outgoing.append(pltpu.make_async_copy(outs.at[2 + j], visit_out.at[j], sems.at[2 + j]))
        outgoing[-1].start()
    for b in range(2):
        outgoing.append(pltpu.make_async_copy(outs.at[b], home_out.at[b], sems.at[b]))
        outgoing[-1].start()
    for copy in outgoing:
        copy.wait()


HBM = pl.BlockSpec(memory_space=pl.ANY)
VMEM = pl.BlockSpec(memory_space=pltpu.VMEM)


def pair_terms(own, other, visit):
    return pl.pallas_call(
        pair_kernel,
        out_shape=(
            jax.ShapeDtypeStruct((2, 2, HALF, PLANE), jnp.float32),
            jax.ShapeDtypeStruct((3, 2, HALF, PLANE), jnp.float32),
        ),
        in_specs=[HBM, HBM, HBM] + [VMEM] * 6,
        out_specs=(HBM, HBM),
        scratch_shapes=[
            pltpu.VMEM((5, 2, HALF, PLANE), jnp.float32),
            pltpu.VMEM((5, 2, HALF, PLANE), jnp.float32),
            pltpu.VMEM((8, 2, 2 * LANES, 2 * LANES), jnp.float32),
            pltpu.VMEM((8, 2, 2 * LANES, 2 * LANES), jnp.float32),
            pltpu.VMEM((ROWS, LANES), jnp.float32),
            pltpu.VMEM((2, N, 41 * LANES), jnp.float32),
            pltpu.VMEM((2, ROWS, LANES), jnp.float32),
            pltpu.SemaphoreType.DMA((7,)),
        ],
        compiler_params=pltpu.CompilerParams(vmem_limit_bytes=60 * 1024 * 1024),
        name="pair_terms",
    )(own, other, visit, *constants())


def places():
    n, g, count = lax.axis_index("band"), lax.axis_index("grid"), lax.axis_size("band")
    core = lax.rem(n, 2)
    swap = (n, 1 - g)
    x_to, x_from = (lax.rem(n + 2, count), 1 - g), (lax.rem(n + count - 2, count), 1 - g)
    y_to, y_from = (lax.rem(n + 1 + 2 * core, count), g), (lax.rem(n + count - 3 + 2 * core, count), g)
    side = (n + 1 - 2 * core, g)
    return g, swap, x_to, x_from, y_to, y_from, side


def meet(receivers):
    barrier = pltpu.get_barrier_semaphore()
    for device in receivers:
        pl.semaphore_signal(barrier, inc=1, device_id=device, device_id_type=MESH)
    pl.semaphore_wait(barrier, len(receivers))


def sender(send, recv):
    index = iter(range(64))

    def make(src, dst, device):
        i = next(index)
        return pltpu.make_async_remote_copy(src, dst, send.at[i], recv.at[i], device_id=device, device_id_type=MESH)

    return make


def gather_kernel(bands, other, visit, send, recv):
    g, swap, x_to, x_from, y_to, y_from, side = places()
    meet([swap, x_from, y_from, side])
    make = sender(send, recv)
    f = 1 - g

    def cells(c):
        return pl.ds(*CHUNKS[c])

    pieces = range(len(CHUNKS))
    e1 = [make(bands.at[g, :, cells(c)], other.at[g, :, cells(c)], swap) for c in pieces]
    x1 = make(bands.at[f], visit.at[0, g], x_to)
    y1 = make(bands.at[f], visit.at[2, g], y_to)
    e2 = make(bands.at[f], other.at[f], swap)
    x2 = [make(other.at[f, :, cells(c)], visit.at[0, f, :, cells(c)], x_to) for c in pieces]
    y2 = [make(other.at[f, :, cells(c)], visit.at[2, f, :, cells(c)], y_to) for c in pieces]
    s1 = make(visit.at[0, f], visit.at[1, f], side)
    s2 = [make(visit.at[0, g, :, cells(c)], visit.at[1, g, :, cells(c)], side) for c in pieces]
    for copy in e1 + [x1, y1]:
        copy.start()
    for c in pieces:
        e1[c].wait_recv()
        x2[c].start()
        y2[c].start()
    e2.start()
    x1.wait_recv()
    s1.start()
    for c in pieces:
        x2[c].wait_recv()
        s2[c].start()
    y1.wait_recv()
    for copy in y2 + [e2, s1] + s2:
        copy.wait_recv()
    for copy in e1 + [x1, y1, e2] + x2 + y2 + [s1] + s2:
        copy.wait_send()


def gathered(bands):
    return pl.pallas_call(
        gather_kernel,
        out_shape=(
            jax.ShapeDtypeStruct((2, HALF, PLANE), jnp.float32),
            jax.ShapeDtypeStruct((3, 2, HALF, PLANE), jnp.float32),
        ),
        in_specs=[HBM],
        out_specs=(HBM, HBM),
        scratch_shapes=[pltpu.SemaphoreType.DMA((16,)), pltpu.SemaphoreType.DMA((16,))],
        compiler_params=pltpu.CompilerParams(collective_id=0, has_side_effects=True),
        name="gather_bands",
    )(bands)


def scatter_kernel(home, visit, out, near, from_s, from_x, from_y, mine, from_e, send, recv, local):
    g, swap, x_to, x_from, y_to, y_from, side = places()
    f = 1 - g
    loads = [pltpu.make_async_copy(visit.at[0], near, local.at[0])]
    loads += [pltpu.make_async_copy(home.at[b], mine.at[b], local.at[1 + b]) for b in range(2)]
    for copy in loads:
        copy.start()
    meet([swap, x_to, y_to, side])
    make = sender(send, recv)
    pieces = range(len(CHUNKS))

    def cells(c):
        return pl.ds(*CHUNKS[c])

    s = [[make(visit.at[1, h, :, cells(c)], from_s.at[h, :, cells(c)], side) for c in pieces] for h in (g, f)]
    y = [make(visit.at[2, h], from_y.at[h], y_from) for h in (f, g)]
    x = [[make(near.at[h, :, cells(c)], from_x.at[h, :, cells(c)], x_from) for c in pieces] for h in (g, f)]
    e1 = make(home.at[g, f], from_e.at[g], swap)
    e2 = [make(mine.at[f, f, :, cells(c)], from_e.at[f, :, cells(c)], swap) for c in pieces]
    for copy in s[0] + [e1] + s[1] + y:
        copy.start()
    loads[0].wait()
    for k, h in enumerate((g, f)):
        for c in pieces:
            s[k][c].wait_recv()
            near[h, :, cells(c)] += from_s[h, :, cells(c)]
            x[k][c].start()
    loads[1].wait()
    loads[2].wait()
    for k, h in enumerate((f, g)):
        y[k].wait_recv()
        for c in pieces:
            x[k][c].wait_recv()
            mine[f, h, :, cells(c)] += from_x[h, :, cells(c)] + from_y[h, :, cells(c)]
            if k == 0:
                e2[c].start()
    e1.wait_recv()
    mine[f, g] += from_e[f]
    outgoing = [pltpu.make_async_copy(mine.at[b, g], out.at[b], local.at[i]) for i, b in enumerate((f, g))]
    outgoing[0].start()
    for c in pieces:
        e2[c].wait_recv()
        mine[g, g, :, cells(c)] += from_e[g, :, cells(c)]
    outgoing[1].start()
    for copy in outgoing:
        copy.wait()
    for copy in s[0] + s[1] + y + x[0] + x[1] + [e1] + e2:
        copy.wait_send()


def scattered(home, visit):
    band = pltpu.VMEM((2, HALF, PLANE), jnp.float32)
    return pl.pallas_call(
        scatter_kernel,
        out_shape=jax.ShapeDtypeStruct((2, HALF, PLANE), jnp.float32),
        in_specs=[HBM, HBM],
        out_specs=HBM,
        scratch_shapes=[
            band, band, band, band, pltpu.VMEM((2, 2, HALF, PLANE), jnp.float32), band,
            pltpu.SemaphoreType.DMA((18,)), pltpu.SemaphoreType.DMA((18,)), pltpu.SemaphoreType.DMA((3,)),
        ],
        compiler_params=pltpu.CompilerParams(collective_id=1, has_side_effects=True, vmem_limit_bytes=60 * 1024 * 1024),
        name="scatter_terms",
    )(home, visit)


def local(bands):
    other, visit = gathered(bands)
    home, parts = pair_terms(bands, other, visit)
    return scattered(home, parts)


def solution(mesh):
    return jax.shard_map(
        local,
        mesh=mesh,
        in_specs=(P("band", "grid", None),),
        out_specs=P("band", "grid", None),
        check_vma=False,
    )
```

```python
import functools
import math

import jax
import jax.numpy as jnp
import numpy as np
from jax import lax
from jax.experimental import pallas as pl
from jax.experimental.pallas import tpu as pltpu
from jax.sharding import PartitionSpec as P

N = 72
HALF = 36
LANES = 128
ROWS = N * N
PLANE = N * N
MESH = pl.DeviceIdType.MESH
PADDED = 80
CHUNKS = ((0, 1792), (1792, 1792), (3584, 1600))
STRIP = 8
spacing = 0.5167


def rounded(x):
    return x.astype(jnp.bfloat16).astype(np.float32)


def constants():
    index = np.arange(N)
    freq = np.where(index <= HALF, index, index - HALF)
    phase = (freq[:, None] * index[None, :] % N) * (2.0 * math.pi / N)
    table = np.where(index[:, None] <= HALF, np.cos(phase), np.sin(phase)).astype(np.float32)

    def stacked(t):
        return np.concatenate([t, t, t - rounded(t)], axis=1)

    def blocks(m):
        wide = np.zeros((2 * N, 2 * LANES), np.float32)
        wide[:N, :N] = m
        wide[N:, LANES : LANES + N] = m
        return np.stack([rounded(wide), rounded(wide - rounded(wide))])

    halves = np.concatenate([np.arange(HALF), np.arange(HALF) + PADDED // 2])
    halved = np.zeros((N, PADDED), np.float32)
    halved[:, halves] = table
    return stacked(table), stacked(table.T), stacked(halved), stacked(halved.T), blocks(table.T), blocks(table.T).transpose(0, 2, 1)


def dot(a, b):
    return jnp.dot(a, b, preferred_element_type=jnp.float32, precision=lax.Precision.DEFAULT)


def low_part(x):
    return x - x.astype(jnp.bfloat16).astype(jnp.float32)


def down(table, x):
    return dot(table, jnp.concatenate([x, low_part(x), x], axis=0))


def joined(x):
    gap = jnp.zeros((PADDED // 2 - HALF, x[0].shape[1]), jnp.float32)
    return jnp.concatenate([x[0], gap, x[1], gap], axis=0)


def along(x, high, low):
    return dot(x, high) + dot(low_part(x), high) + dot(x, low)


def fill_tables(wide_ahead, wide_back, lane_ahead, lane_back, factors):
    rows = lax.broadcasted_iota(jnp.int32, (2 * N, 2 * LANES), 0)
    cols = lax.broadcasted_iota(jnp.int32, (2 * N, 2 * LANES), 1)
    for u in range(8):
        start = 2 * N * u % LANES
        move = jnp.where(cols == rows + start, 1.0, 0.0)
        for part in range(2):
            lane_ahead[u, part] = jnp.zeros((2 * LANES, 2 * LANES), jnp.float32)
            lane_ahead[u, part, start : start + 2 * N, :] = wide_ahead[part]
            lane_back[u, part] = dot(wide_back[part], move)

    def wave(i):
        f = jnp.where(i <= HALF, i, i - HALF)
        return (f * f).astype(jnp.float32), jnp.where((i == 0) | (i == HALF), 1.0, 2.0).astype(jnp.float32)

    factor = (2.0 * math.pi / (N * spacing)) ** 2
    square_b, weight_b = wave(lax.broadcasted_iota(jnp.int32, (N, LANES), 0))
    square_c, weight_c = wave(lax.broadcasted_iota(jnp.int32, (N, LANES), 1))
    inside = lax.broadcasted_iota(jnp.int32, (N, LANES), 1) < N

    def fill(i, _):
        square_a, weight_a = wave(i)
        ksq = factor * (square_a + square_b + square_c)
        keep = (ksq > 0) & inside
        coulomb = jnp.where(keep, 4.0 * math.pi / jnp.where(keep, ksq, 1.0), 0.0)
        factors[pl.ds(pl.multiple_of(i * N, 8), N), :] = coulomb * (weight_a * weight_b * weight_c) / float(N**3)
        return 0

    lax.fori_loop(0, N, fill, 0)


def exchange(homes, visit, home_outs, visit_out, first, tables, lane_ahead, lane_back, factors, u, w):
    ahead, back, half_ahead, half_back = tables
    BODY = 5
    WIDE = 2 * LANES
    TAIL = PLANE // WIDE * WIDE

    def flat_ahead(tiles):
        for at, width in tiles:
            for p in range(2):
                x = joined([homes[p][h, :, pl.ds(at, width)] * visit[h, :, pl.ds(at, width)] for h in range(2)])
                if width < LANES:
                    x = jnp.concatenate([x, jnp.zeros((PADDED, LANES - width), jnp.float32)], axis=1)
                u[p, :, pl.ds(at, max(width, LANES))] = down(half_ahead[...], x)

    def wide_tiles(i):
        return [(pl.multiple_of((i * BODY + k) * WIDE, LANES), WIDE) for k in range(BODY)]

    def pass_1(i, _):
        flat_ahead(wide_tiles(i))
        return 0

    lax.fori_loop(0, TAIL // WIDE // BODY, pass_1, 0)
    flat_ahead([(TAIL, PLANE - TAIL)])

    def lines_ahead(t, count):
        base = pl.multiple_of(t * 9 * LANES, LANES)
        for k in range(count):
            at = 2 * N * k // LANES * LANES
            x = jnp.concatenate([u[p, :, pl.ds(base + at, WIDE)] for p in range(2)], axis=0)
            y = along(x, lane_ahead[k, 0], lane_ahead[k, 1])
            r = pl.multiple_of((t * 8 + k) * 2 * N, 8)
            for p in range(2):
                w[p, pl.ds(r, N), :] = y[N * p : N * (p + 1), :LANES]
                w[p, pl.ds(r + N, N), :] = y[N * p : N * (p + 1), LANES:]

    def pass_2(t, _):
        lines_ahead(t, 8)
        return 0

    lax.fori_loop(0, 4, pass_2, 0)
    lines_ahead(4, 4)

    def load_w(i):
        rows = pl.ds(i, N, stride=N)
        return jnp.concatenate([w[0, rows, :], w[1, rows, :]], axis=1)

    def store_w(i, y):
        rows = pl.ds(i, N, stride=N)
        w[0, rows, :] = y[:, :LANES]
        w[1, rows, :] = y[:, LANES:]

    def ahead_b(i, x):
        y = down(ahead[...], x)
        f = factors[pl.ds(pl.multiple_of(i * N, 8), N), :]
        return y * jnp.concatenate([f, f], axis=1)

    def pass_3(i, _):
        now = [i * STRIP + k for k in range(STRIP)]
        before = [i * STRIP - STRIP + k for k in range(STRIP)]
        xs, ys = [load_w(q) for q in now], [load_w(q) for q in before]
        xs = [ahead_b(q, x) for q, x in zip(now, xs)]
        ys = [down(back[...], y) for y in ys]
        for q, x in zip(now, xs):
            store_w(q, x)
        for q, y in zip(before, ys):
            store_w(q, y)
        return 0

    for q, x in [(q, ahead_b(q, load_w(q))) for q in range(STRIP)]:
        store_w(q, x)
    lax.fori_loop(1, N // STRIP, pass_3, 0)
    for q, y in [(q, down(back[...], load_w(q))) for q in range(N - STRIP, N)]:
        store_w(q, y)

    def lines_back(t, count):
        base = pl.multiple_of(t * 9 * LANES, LANES)
        total = {}
        for k in range(count):
            tile = 2 * N * k // LANES
            r = pl.multiple_of((t * 8 + k) * 2 * N, 8)
            x = jnp.concatenate(
                [jnp.concatenate([w[p, pl.ds(r, N), :], w[p, pl.ds(r + N, N), :]], axis=1) for p in range(2)], axis=0
            )
            y = along(x, lane_back[k, 0], lane_back[k, 1])
            for half in range(2):
                part = y[:, LANES * half : LANES * (half + 1)]
                total[tile + half] = total[tile + half] + part if tile + half in total else part
        for tile, value in total.items():
            for p in range(2):
                u[p, :, pl.ds(base + tile * LANES, LANES)] = value[N * p : N * (p + 1)]

    def pass_4(t, _):
        lines_back(t, 8)
        return 0

    lax.fori_loop(0, 4, pass_4, 0)
    lines_back(4, 4)

    def flat_back(tiles):
        for at, width in tiles:
            cells = pl.ds(at, width)
            total = [0.0, 0.0]
            for p in range(2):
                v = down(half_back[...], u[p, :, pl.ds(at, max(width, LANES))])[:, :width]
                for h in range(2):
                    part = v[PADDED // 2 * h : PADDED // 2 * h + HALF]
                    mine = part * visit[h, :, cells]
                    home_outs[p][h, :, cells] = -mine if first else home_outs[p][h, :, cells] - mine
                    total[h] = total[h] - part * homes[p][h, :, cells]
            for h in range(2):
                visit_out[h, :, cells] = total[h]

    def pass_5(i, _):
        flat_back(wide_tiles(i))
        return 0

    lax.fori_loop(0, TAIL // WIDE // BODY, pass_5, 0)
    flat_back([(TAIL, PLANE - TAIL)])


def pair_kernel(
    own, other, visit_in, ahead, back, half_ahead, half_back, wide_ahead, wide_back, home_out, visit_out,
    flat, outs, lane_ahead, lane_back, factors, u, w, sems,
):
    g = lax.axis_index("grid")
    copies = [pltpu.make_async_copy(own.at[b], flat.at[b, g], sems.at[b]) for b in range(2)]
    copies += [pltpu.make_async_copy(other.at[b], flat.at[b, 1 - g], sems.at[2 + b]) for b in range(2)]
    copies += [pltpu.make_async_copy(visit_in.at[i], flat.at[2 + i], sems.at[4 + i]) for i in range(3)]
    for copy in copies:
        copy.start()
    fill_tables(wide_ahead, wide_back, lane_ahead, lane_back, factors)
    for copy in copies:
        copy.wait()
    outgoing = []
    for j in range(3):
        exchange(
            [flat.at[0], flat.at[1]], flat.at[2 + j], [outs.at[0], outs.at[1]], outs.at[2 + j], j == 0,
            (ahead, back, half_ahead, half_back), lane_ahead, lane_back, factors, u, w,
        )
        outgoing.append(pltpu.make_async_copy(outs.at[2 + j], visit_out.at[j], sems.at[2 + j]))
        outgoing[-1].start()
    for b in range(2):
        outgoing.append(pltpu.make_async_copy(outs.at[b], home_out.at[b], sems.at[b]))
        outgoing[-1].start()
    for copy in outgoing:
        copy.wait()


HBM = pl.BlockSpec(memory_space=pl.ANY)
VMEM = pl.BlockSpec(memory_space=pltpu.VMEM)


def pair_terms(own, other, visit):
    return pl.pallas_call(
        pair_kernel,
        out_shape=(
            jax.ShapeDtypeStruct((2, 2, HALF, PLANE), jnp.float32),
            jax.ShapeDtypeStruct((3, 2, HALF, PLANE), jnp.float32),
        ),
        in_specs=[HBM, HBM, HBM] + [VMEM] * 6,
        out_specs=(HBM, HBM),
        scratch_shapes=[
            pltpu.VMEM((5, 2, HALF, PLANE), jnp.float32),
            pltpu.VMEM((5, 2, HALF, PLANE), jnp.float32),
            pltpu.VMEM((8, 2, 2 * LANES, 2 * LANES), jnp.float32),
            pltpu.VMEM((8, 2, 2 * LANES, 2 * LANES), jnp.float32),
            pltpu.VMEM((ROWS, LANES), jnp.float32),
            pltpu.VMEM((2, N, 41 * LANES), jnp.float32),
            pltpu.VMEM((2, ROWS, LANES), jnp.float32),
            pltpu.SemaphoreType.DMA((7,)),
        ],
        compiler_params=pltpu.CompilerParams(vmem_limit_bytes=60 * 1024 * 1024),
        name="pair_terms",
    )(own, other, visit, *constants())


def places():
    n, g, count = lax.axis_index("band"), lax.axis_index("grid"), lax.axis_size("band")
    core, r = lax.rem(n, 2), lax.rem(n, 4)
    swap = (n, 1 - g)
    x_to = (lax.rem(n + 2, count), 1 - g)
    x_from = (jnp.where(r == 1, n + 1, lax.rem(n + count - 2, count)), 1 - g)
    r_to = (lax.rem(n + count - 1, count), 1 - g)
    y_to, y_from = (lax.rem(n + 1 + 2 * core, count), g), (lax.rem(n + count - 3 + 2 * core, count), g)
    side = (n + 1 - 2 * core, g)
    return g, r, swap, x_to, x_from, r_to, y_to, y_from, side


def meet(senders, count):
    barrier = pltpu.get_barrier_semaphore()
    for use, device in senders:

        def signal():
            pl.semaphore_signal(barrier, inc=1, device_id=device, device_id_type=MESH)

        signal() if use is None else pl.when(use)(signal)
    pl.semaphore_wait(barrier, count)


def sender(send, recv):
    index = iter(range(64))

    def make(src, dst, device, into=None):
        i = next(index)
        j = i if into is None else into
        copy = pltpu.make_async_remote_copy(src, dst, send.at[i], recv.at[j], device_id=device, device_id_type=MESH)
        return copy, i

    return make


def gather_kernel(bands, other, visit, send, recv):
    g, r, swap, x_to, x_from, r_to, y_to, y_from, side = places()
    sends_x, relays = r != 3, r == 2
    meet(
        [(None, swap), (None, x_from), (None, y_from), (None, side)],
        3 + jnp.where(sends_x, 1, 0) + jnp.where(relays, 1, 0),
    )
    make = sender(send, recv)
    f = 1 - g

    def cells(c):
        return pl.ds(*CHUNKS[c])

    pieces = range(len(CHUNKS))

    def many(src, dst, device, into=None):
        made = [
            make(src.at[:, cells(c)], dst.at[:, cells(c)], device, None if into is None else into[c]) for c in pieces
        ]
        return [copy for copy, _ in made], [i for _, i in made]

    e1, _ = many(bands.at[g], other.at[g], swap)
    x1, x1_at = make(bands.at[f], visit.at[0, g], x_to)
    y1, _ = make(bands.at[f], visit.at[2, g], y_to)
    e2, _ = make(bands.at[f], other.at[f], swap)
    x2, x2_at = many(other.at[f], visit.at[0, f], x_to)
    y2, _ = many(other.at[f], visit.at[2, f], y_to)
    s1, _ = make(visit.at[0, f], visit.at[1, f], side)
    s2, _ = many(visit.at[0, g], visit.at[1, g], side)
    r1, _ = make(visit.at[2, g], visit.at[0, g], r_to, x1_at)
    r2, _ = many(visit.at[2, f], visit.at[0, f], r_to, x2_at)
    for copy in e1:
        copy.start()

    @pl.when(sends_x)
    def _():
        x1.start()

    y1.start()
    for c in pieces:
        e1[c].wait_recv()

        @pl.when(sends_x)
        def _():
            x2[c].start()

        y2[c].start()
    e2.start()
    y1.wait_recv()

    @pl.when(relays)
    def _():
        r1.start()

    @pl.when(relays)
    def _():
        for c in pieces:
            y2[c].wait_recv()
            r2[c].start()

    x1.wait_recv()
    s1.start()
    for c in pieces:
        x2[c].wait_recv()
        s2[c].start()

    @pl.when(r != 2)
    def _():
        for c in pieces:
            y2[c].wait_recv()

    for copy in [e2, s1] + s2:
        copy.wait_recv()
    for copy in e1 + [y1, e2] + y2 + [s1] + s2:
        copy.wait_send()

    @pl.when(sends_x)
    def _():
        for copy in [x1] + x2:
            copy.wait_send()

    @pl.when(relays)
    def _():
        for copy in [r1] + r2:
            copy.wait_send()


def gathered(bands):
    return pl.pallas_call(
        gather_kernel,
        out_shape=(
            jax.ShapeDtypeStruct((2, HALF, PLANE), jnp.float32),
            jax.ShapeDtypeStruct((3, 2, HALF, PLANE), jnp.float32),
        ),
        in_specs=[HBM],
        out_specs=(HBM, HBM),
        scratch_shapes=[pltpu.SemaphoreType.DMA((20,)), pltpu.SemaphoreType.DMA((20,))],
        compiler_params=pltpu.CompilerParams(collective_id=0, has_side_effects=True),
        name="gather_bands",
    )(bands)


def scatter_kernel(home, visit, out, near, far, from_s, from_x, from_y, from_r, mine, from_e, send, recv, local):
    g, r, swap, x_to, x_from, r_to, y_to, y_from, side = places()
    sent_x, relayed = r != 3, r == 2
    f = 1 - g
    loads = [pltpu.make_async_copy(visit.at[0], near, local.at[0])]
    loads += [pltpu.make_async_copy(home.at[b], mine.at[b], local.at[1 + b]) for b in range(2)]
    loads += [pltpu.make_async_copy(visit.at[2], far, local.at[3])]
    for copy in loads:
        copy.start()
    meet([(None, swap), (sent_x, x_to), (relayed, r_to), (None, y_to), (None, side)], 4)
    make = sender(send, recv)
    pieces = range(len(CHUNKS))

    def cells(c):
        return pl.ds(*CHUNKS[c])

    def many(src, dst, device):
        return [make(src.at[:, cells(c)], dst.at[:, cells(c)], device)[0] for c in pieces]

    s = [many(visit.at[1, h], from_s.at[h], side) for h in (g, f)]
    y = [many(far.at[h], from_y.at[h], y_from) for h in (f, g)]
    x = [many(near.at[h], from_x.at[h], x_from) for h in (g, f)]
    q = [many(near.at[h], from_r.at[h], x_from) for h in (g, f)]
    e1, _ = make(home.at[g, f], from_e.at[g], swap)
    e2 = many(mine.at[f, f], from_e.at[f], swap)
    for copy in s[0] + [e1] + s[1]:
        copy.start()
    loads[3].wait()

    @pl.when(r != 2)
    def _():
        for copy in y[0] + y[1]:
            copy.start()

    loads[0].wait()
    for k, h in enumerate((g, f)):
        for c in pieces:
            s[k][c].wait_recv()
            near[h, :, cells(c)] += from_s[h, :, cells(c)]

            @pl.when(r != 1)
            def _():
                x[k][c].start()

            @pl.when(r == 1)
            def _():
                q[k][c].start()

    @pl.when(relayed)
    def _():
        for k, h in enumerate((f, g)):
            for c in pieces:
                q[k][c].wait_recv()
                far[h, :, cells(c)] += from_r[h, :, cells(c)]
                y[k][c].start()

    loads[1].wait()
    loads[2].wait()
    for k, h in enumerate((f, g)):
        for c in pieces:

            @pl.when(sent_x)
            def _():
                x[k][c].wait_recv()
                mine[f, h, :, cells(c)] += from_x[h, :, cells(c)]

            y[k][c].wait_recv()
            mine[f, h, :, cells(c)] += from_y[h, :, cells(c)]
            if k == 0:
                e2[c].start()
    e1.wait_recv()
    mine[f, g] += from_e[f]
    outgoing = [pltpu.make_async_copy(mine.at[b, g], out.at[b], local.at[i]) for i, b in enumerate((f, g))]
    outgoing[0].start()
    for c in pieces:
        e2[c].wait_recv()
        mine[g, g, :, cells(c)] += from_e[g, :, cells(c)]
    outgoing[1].start()
    for copy in outgoing:
        copy.wait()
    for copy in s[0] + s[1] + y[0] + y[1] + [e1] + e2:
        copy.wait_send()

    @pl.when(r != 1)
    def _():
        for copy in x[0] + x[1]:
            copy.wait_send()

    @pl.when(r == 1)
    def _():
        for copy in q[0] + q[1]:
            copy.wait_send()


def scattered(home, visit):
    band = pltpu.VMEM((2, HALF, PLANE), jnp.float32)
    return pl.pallas_call(
        scatter_kernel,
        out_shape=jax.ShapeDtypeStruct((2, HALF, PLANE), jnp.float32),
        in_specs=[HBM, HBM],
        out_specs=HBM,
        scratch_shapes=[
            band, band, band, band, band, band, pltpu.VMEM((2, 2, HALF, PLANE), jnp.float32), band,
            pltpu.SemaphoreType.DMA((28,)), pltpu.SemaphoreType.DMA((28,)), pltpu.SemaphoreType.DMA((4,)),
        ],
        compiler_params=pltpu.CompilerParams(collective_id=1, has_side_effects=True, vmem_limit_bytes=60 * 1024 * 1024),
        name="scatter_terms",
    )(home, visit)


def local(bands):
    other, visit = gathered(bands)
    home, parts = pair_terms(bands, other, visit)
    return scattered(home, parts)


def solution(mesh):
    return jax.shard_map(
        local,
        mesh=mesh,
        in_specs=(P("band", "grid", None),),
        out_specs=P("band", "grid", None),
        check_vma=False,
    )
```

```python
import functools
import math

import jax
import jax.numpy as jnp
import numpy as np
from jax import lax
from jax.experimental import pallas as pl
from jax.experimental.pallas import tpu as pltpu
from jax.sharding import PartitionSpec as P

N = 72
HALF = 36
LANES = 128
ROWS = N * N
PLANE = N * N
MESH = pl.DeviceIdType.MESH
PADDED = 80
CHUNKS = ((0, 1792), (1792, 1792), (3584, 1600))
STRIP = 8
spacing = 0.5167


def rounded(x):
    return x.astype(jnp.bfloat16).astype(np.float32)


def constants():
    index = np.arange(N)
    freq = np.where(index <= HALF, index, index - HALF)
    phase = (freq[:, None] * index[None, :] % N) * (2.0 * math.pi / N)
    table = np.where(index[:, None] <= HALF, np.cos(phase), np.sin(phase)).astype(np.float32)

    def stacked(t):
        return np.concatenate([t, t, t - rounded(t)], axis=1)

    def blocks(m):
        wide = np.zeros((2 * N, 2 * LANES), np.float32)
        wide[:N, :N] = m
        wide[N:, LANES : LANES + N] = m
        return np.stack([rounded(wide), rounded(wide - rounded(wide))])

    halves = np.concatenate([np.arange(HALF), np.arange(HALF) + PADDED // 2])
    halved = np.zeros((N, PADDED), np.float32)
    halved[:, halves] = table
    return stacked(table), stacked(table.T), stacked(halved), stacked(halved.T), blocks(table.T), blocks(table.T).transpose(0, 2, 1)


def dot(a, b):
    return jnp.dot(a, b, preferred_element_type=jnp.float32, precision=lax.Precision.DEFAULT)


def low_part(x):
    return x - x.astype(jnp.bfloat16).astype(jnp.float32)


def down(table, x):
    return dot(table, jnp.concatenate([x, low_part(x), x], axis=0))


def joined(x):
    gap = jnp.zeros((PADDED // 2 - HALF, x[0].shape[1]), jnp.float32)
    return jnp.concatenate([x[0], gap, x[1], gap], axis=0)


def along(x, high, low):
    return dot(x, high) + dot(low_part(x), high) + dot(x, low)


def fill_tables(wide_ahead, wide_back, lane_ahead, lane_back, factors):
    rows = lax.broadcasted_iota(jnp.int32, (2 * N, 2 * LANES), 0)
    cols = lax.broadcasted_iota(jnp.int32, (2 * N, 2 * LANES), 1)
    for u in range(8):
        start = 2 * N * u % LANES
        move = jnp.where(cols == rows + start, 1.0, 0.0)
        for part in range(2):
            lane_ahead[u, part] = jnp.zeros((2 * LANES, 2 * LANES), jnp.float32)
            lane_ahead[u, part, start : start + 2 * N, :] = wide_ahead[part]
            lane_back[u, part] = dot(wide_back[part], move)

    def wave(i):
        f = jnp.where(i <= HALF, i, i - HALF)
        return (f * f).astype(jnp.float32), jnp.where((i == 0) | (i == HALF), 1.0, 2.0).astype(jnp.float32)

    factor = (2.0 * math.pi / (N * spacing)) ** 2
    square_b, weight_b = wave(lax.broadcasted_iota(jnp.int32, (N, LANES), 0))
    square_c, weight_c = wave(lax.broadcasted_iota(jnp.int32, (N, LANES), 1))
    inside = lax.broadcasted_iota(jnp.int32, (N, LANES), 1) < N

    def fill(i, _):
        square_a, weight_a = wave(i)
        ksq = factor * (square_a + square_b + square_c)
        keep = (ksq > 0) & inside
        coulomb = jnp.where(keep, 4.0 * math.pi / jnp.where(keep, ksq, 1.0), 0.0)
        factors[pl.ds(pl.multiple_of(i * N, 8), N), :] = coulomb * (weight_a * weight_b * weight_c) / float(N**3)
        return 0

    lax.fori_loop(0, N, fill, 0)


def exchange(homes, visit, home_outs, visit_out, first, tables, lane_ahead, lane_back, factors, u, w):
    ahead, back, half_ahead, half_back = tables
    BODY = 5
    WIDE = 2 * LANES
    TAIL = PLANE // WIDE * WIDE

    def flat_ahead(tiles):
        for at, width in tiles:
            for p in range(2):
                x = joined([homes[p][h, :, pl.ds(at, width)] * visit[h, :, pl.ds(at, width)] for h in range(2)])
                if width < LANES:
                    x = jnp.concatenate([x, jnp.zeros((PADDED, LANES - width), jnp.float32)], axis=1)
                u[p, :, pl.ds(at, max(width, LANES))] = down(half_ahead[...], x)

    def wide_tiles(i):
        return [(pl.multiple_of((i * BODY + k) * WIDE, LANES), WIDE) for k in range(BODY)]

    def pass_1(i, _):
        flat_ahead(wide_tiles(i))
        return 0

    lax.fori_loop(0, TAIL // WIDE // BODY, pass_1, 0)
    flat_ahead([(TAIL, PLANE - TAIL)])

    def lines_ahead(t, count):
        base = pl.multiple_of(t * 9 * LANES, LANES)
        for k in range(count):
            at = 2 * N * k // LANES * LANES
            x = jnp.concatenate([u[p, :, pl.ds(base + at, WIDE)] for p in range(2)], axis=0)
            y = along(x, lane_ahead[k, 0], lane_ahead[k, 1])
            r = pl.multiple_of((t * 8 + k) * 2 * N, 8)
            for p in range(2):
                w[p, pl.ds(r, N), :] = y[N * p : N * (p + 1), :LANES]
                w[p, pl.ds(r + N, N), :] = y[N * p : N * (p + 1), LANES:]

    def pass_2(t, _):
        lines_ahead(t, 8)
        return 0

    lax.fori_loop(0, 4, pass_2, 0)
    lines_ahead(4, 4)

    def load_w(i):
        rows = pl.ds(i, N, stride=N)
        return jnp.concatenate([w[0, rows, :], w[1, rows, :]], axis=1)

    def store_w(i, y):
        rows = pl.ds(i, N, stride=N)
        w[0, rows, :] = y[:, :LANES]
        w[1, rows, :] = y[:, LANES:]

    def ahead_b(i, x):
        y = down(ahead[...], x)
        f = factors[pl.ds(pl.multiple_of(i * N, 8), N), :]
        return y * jnp.concatenate([f, f], axis=1)

    def pass_3(i, _):
        now = [i * STRIP + k for k in range(STRIP)]
        before = [i * STRIP - STRIP + k for k in range(STRIP)]
        xs, ys = [load_w(q) for q in now], [load_w(q) for q in before]
        xs = [ahead_b(q, x) for q, x in zip(now, xs)]
        ys = [down(back[...], y) for y in ys]
        for q, x in zip(now, xs):
            store_w(q, x)
        for q, y in zip(before, ys):
            store_w(q, y)
        return 0

    for q, x in [(q, ahead_b(q, load_w(q))) for q in range(STRIP)]:
        store_w(q, x)
    lax.fori_loop(1, N // STRIP, pass_3, 0)
    for q, y in [(q, down(back[...], load_w(q))) for q in range(N - STRIP, N)]:
        store_w(q, y)

    def lines_back(t, count):
        base = pl.multiple_of(t * 9 * LANES, LANES)
        total = {}
        for k in range(count):
            tile = 2 * N * k // LANES
            r = pl.multiple_of((t * 8 + k) * 2 * N, 8)
            x = jnp.concatenate(
                [jnp.concatenate([w[p, pl.ds(r, N), :], w[p, pl.ds(r + N, N), :]], axis=1) for p in range(2)], axis=0
            )
            y = along(x, lane_back[k, 0], lane_back[k, 1])
            for half in range(2):
                part = y[:, LANES * half : LANES * (half + 1)]
                total[tile + half] = total[tile + half] + part if tile + half in total else part
        for tile, value in total.items():
            for p in range(2):
                u[p, :, pl.ds(base + tile * LANES, LANES)] = value[N * p : N * (p + 1)]

    def pass_4(t, _):
        lines_back(t, 8)
        return 0

    lax.fori_loop(0, 4, pass_4, 0)
    lines_back(4, 4)

    def flat_back(tiles):
        for at, width in tiles:
            cells = pl.ds(at, width)
            total = [0.0, 0.0]
            for p in range(2):
                v = down(half_back[...], u[p, :, pl.ds(at, max(width, LANES))])[:, :width]
                for h in range(2):
                    part = v[PADDED // 2 * h : PADDED // 2 * h + HALF]
                    mine = part * visit[h, :, cells]
                    home_outs[p][h, :, cells] = -mine if first else home_outs[p][h, :, cells] - mine
                    total[h] = total[h] - part * homes[p][h, :, cells]
            for h in range(2):
                visit_out[h, :, cells] = total[h]

    def pass_5(i, _):
        flat_back(wide_tiles(i))
        return 0

    lax.fori_loop(0, TAIL // WIDE // BODY, pass_5, 0)
    flat_back([(TAIL, PLANE - TAIL)])


HBM = pl.BlockSpec(memory_space=pl.ANY)
VMEM = pl.BlockSpec(memory_space=pltpu.VMEM)


def places():
    n, g, count = lax.axis_index("band"), lax.axis_index("grid"), lax.axis_size("band")
    core, r = lax.rem(n, 2), lax.rem(n, 4)
    swap = (n, 1 - g)
    x_to = (lax.rem(n + 2, count), 1 - g)
    x_from = (jnp.where(r == 1, n + 1, lax.rem(n + count - 2, count)), 1 - g)
    r_to = (lax.rem(n + count - 1, count), 1 - g)
    y_to, y_from = (lax.rem(n + 1 + 2 * core, count), g), (lax.rem(n + count - 3 + 2 * core, count), g)
    side = (n + 1 - 2 * core, g)
    return g, r, swap, x_to, x_from, r_to, y_to, y_from, side


def meet(senders, count):
    barrier = pltpu.get_barrier_semaphore()
    for use, device in senders:

        def signal():
            pl.semaphore_signal(barrier, inc=1, device_id=device, device_id_type=MESH)

        signal() if use is None else pl.when(use)(signal)
    pl.semaphore_wait(barrier, count)


def sender(send, recv):
    index = iter(range(64))

    def make(src, dst, device, into=None):
        i = next(index)
        j = i if into is None else into
        copy = pltpu.make_async_remote_copy(src, dst, send.at[i], recv.at[j], device_id=device, device_id_type=MESH)
        return copy, i

    return make


def exchange_kernel(
    bands, ahead, back, half_ahead, half_back, wide_ahead, wide_back, out,
    flat, outs, lane_ahead, lane_back, factors, u, w, from_s, from_x, from_y, from_r, from_e, send, recv, local,
):
    g, r, swap, x_to, x_from, r_to, y_to, y_from, side = places()
    sends_x, relays = r != 3, r == 2
    f = 1 - g
    pieces = range(len(CHUNKS))
    make = sender(send, recv)

    def cells(c):
        return pl.ds(*CHUNKS[c])

    def many(src, dst, device, into=None):
        made = [
            make(src.at[:, cells(c)], dst.at[:, cells(c)], device, None if into is None else into[c]) for c in pieces
        ]
        return [copy for copy, _ in made], [i for _, i in made]

    meet(
        [(None, swap), (None, x_from), (None, y_from), (None, side)],
        3 + jnp.where(sends_x, 1, 0) + jnp.where(relays, 1, 0),
    )
    e1, _ = many(bands.at[g], flat.at[g, g], swap)
    x1, x1_at = make(bands.at[f], flat.at[2, g], x_to)
    y1, _ = make(bands.at[f], flat.at[4, g], y_to)
    e2, _ = make(bands.at[f], flat.at[f, g], swap)
    x2, x2_at = many(flat.at[f, f], flat.at[2, f], x_to)
    y2, _ = many(flat.at[f, f], flat.at[4, f], y_to)
    s1, _ = make(flat.at[2, f], flat.at[3, f], side)
    s2, _ = many(flat.at[2, g], flat.at[3, g], side)
    r1, _ = make(flat.at[4, g], flat.at[2, g], r_to, x1_at)
    r2, _ = many(flat.at[4, f], flat.at[2, f], r_to, x2_at)
    loads = [pltpu.make_async_copy(bands.at[b], flat.at[b, g], local.at[b]) for b in range(2)]
    for copy in e1:
        copy.start()

    @pl.when(sends_x)
    def _():
        x1.start()

    y1.start()
    for copy in loads:
        copy.start()
    fill_tables(wide_ahead, wide_back, lane_ahead, lane_back, factors)
    for c in pieces:
        e1[c].wait_recv()

        @pl.when(sends_x)
        def _():
            x2[c].start()

        y2[c].start()
    e2.start()
    y1.wait_recv()

    @pl.when(relays)
    def _():
        r1.start()
        for c in pieces:
            y2[c].wait_recv()
            r2[c].start()

    x1.wait_recv()
    s1.start()
    for c in pieces:
        x2[c].wait_recv()
        s2[c].start()
    for copy in loads:
        copy.wait()
    e2.wait_recv()

    def pairs(slot, first):
        exchange(
            [flat.at[0], flat.at[1]], flat.at[slot], [outs.at[0], outs.at[1]], outs.at[slot], first,
            (ahead, back, half_ahead, half_back), lane_ahead, lane_back, factors, u, w,
        )

    s_back = [many(outs.at[3, h], from_s.at[h], side)[0] for h in (g, f)]
    y_back = [many(outs.at[4, h], from_y.at[h], y_from)[0] for h in (f, g)]
    x_back = [many(outs.at[2, h], from_x.at[h], x_from)[0] for h in (g, f)]
    r_back = [many(outs.at[2, h], from_r.at[h], x_from)[0] for h in (g, f)]
    e1_back, _ = make(outs.at[g, f], from_e.at[g], swap)
    e2_back, _ = many(outs.at[f, f], from_e.at[f], swap)

    pairs(2, True)
    s1.wait_recv()
    for copy in s2:
        copy.wait_recv()
    pairs(3, False)
    for copy in s_back[0] + s_back[1]:
        copy.start()
    for k, h in enumerate((g, f)):
        for c in pieces:
            s_back[k][c].wait_recv()
            outs[2, h, :, cells(c)] += from_s[h, :, cells(c)]

            @pl.when(r != 1)
            def _():
                x_back[k][c].start()

            @pl.when(r == 1)
            def _():
                r_back[k][c].start()

    @pl.when(r != 2)
    def _():
        for c in pieces:
            y2[c].wait_recv()

    pairs(4, False)
    e1_back.start()

    @pl.when(r != 2)
    def _():
        for copy in y_back[0] + y_back[1]:
            copy.start()

    @pl.when(relays)
    def _():
        for k, h in enumerate((f, g)):
            for c in pieces:
                r_back[k][c].wait_recv()
                outs[4, h, :, cells(c)] += from_r[h, :, cells(c)]
                y_back[k][c].start()

    for k, h in enumerate((f, g)):
        for c in pieces:

            @pl.when(sends_x)
            def _():
                x_back[k][c].wait_recv()
                outs[f, h, :, cells(c)] += from_x[h, :, cells(c)]

            y_back[k][c].wait_recv()
            outs[f, h, :, cells(c)] += from_y[h, :, cells(c)]
            if k == 0:
                e2_back[c].start()
    e1_back.wait_recv()
    outs[f, g] += from_e[f]
    stores = [pltpu.make_async_copy(outs.at[b, g], out.at[b], local.at[i]) for i, b in enumerate((f, g))]
    stores[0].start()
    for c in pieces:
        e2_back[c].wait_recv()
        outs[g, g, :, cells(c)] += from_e[g, :, cells(c)]
    stores[1].start()
    for copy in stores:
        copy.wait()
    for copy in e1 + [y1, e2] + y2 + [s1] + s2 + s_back[0] + s_back[1] + y_back[0] + y_back[1] + [e1_back] + e2_back:
        copy.wait_send()

    @pl.when(sends_x)
    def _():
        for copy in [x1] + x2:
            copy.wait_send()

    @pl.when(relays)
    def _():
        for copy in [r1] + r2:
            copy.wait_send()

    @pl.when(r != 1)
    def _():
        for copy in x_back[0] + x_back[1]:
            copy.wait_send()

    @pl.when(r == 1)
    def _():
        for copy in r_back[0] + r_back[1]:
            copy.wait_send()


def local(bands):
    band = pltpu.VMEM((2, HALF, PLANE), jnp.float32)
    table = pltpu.VMEM((8, 2, 2 * LANES, 2 * LANES), jnp.float32)
    return pl.pallas_call(
        exchange_kernel,
        out_shape=jax.ShapeDtypeStruct((2, HALF, PLANE), jnp.float32),
        in_specs=[HBM] + [VMEM] * 6,
        out_specs=HBM,
        scratch_shapes=[
            pltpu.VMEM((5, 2, HALF, PLANE), jnp.float32),
            pltpu.VMEM((5, 2, HALF, PLANE), jnp.float32),
            table, table,
            pltpu.VMEM((ROWS, LANES), jnp.float32),
            pltpu.VMEM((2, N, 41 * LANES), jnp.float32),
            pltpu.VMEM((2, ROWS, LANES), jnp.float32),
            band, band, band, band, band,
            pltpu.SemaphoreType.DMA((48,)), pltpu.SemaphoreType.DMA((48,)), pltpu.SemaphoreType.DMA((2,)),
        ],
        compiler_params=pltpu.CompilerParams(collective_id=0, has_side_effects=True, vmem_limit_bytes=63 * 1024 * 1024),
        name="exchange_terms",
    )(bands, *constants())


def solution(mesh):
    return jax.shard_map(
        local,
        mesh=mesh,
        in_specs=(P("band", "grid", None),),
        out_specs=P("band", "grid", None),
        check_vma=False,
    )
```

```python
import functools
import math

import jax
import jax.numpy as jnp
import numpy as np
from jax import lax
from jax.experimental import pallas as pl
from jax.experimental.pallas import tpu as pltpu
from jax.sharding import PartitionSpec as P

N = 72
HALF = 36
LANES = 128
ROWS = N * N
PLANE = N * N
MESH = pl.DeviceIdType.MESH
PADDED = 80
CHUNKS = ((0, 1792), (1792, 1792), (3584, 1600))
STRIP = 12
spacing = 0.5167


def rounded(x):
    return x.astype(jnp.bfloat16).astype(np.float32)


def constants():
    index = np.arange(N)
    freq = np.where(index <= HALF, index, index - HALF)
    phase = (freq[:, None] * index[None, :] % N) * (2.0 * math.pi / N)
    table = np.where(index[:, None] <= HALF, np.cos(phase), np.sin(phase)).astype(np.float32)

    def stacked(t):
        return np.concatenate([t, t, t - rounded(t)], axis=1)

    def blocks(m):
        wide = np.zeros((2 * N, 2 * LANES), np.float32)
        wide[:N, :N] = m
        wide[N:, LANES : LANES + N] = m
        return np.stack([rounded(wide), rounded(wide - rounded(wide))])

    halves = np.concatenate([np.arange(HALF), np.arange(HALF) + PADDED // 2])
    halved = np.zeros((N, PADDED), np.float32)
    halved[:, halves] = table
    return stacked(table), stacked(table.T), stacked(halved), stacked(halved.T), blocks(table.T), blocks(table.T).transpose(0, 2, 1)


def dot(a, b):
    return jnp.dot(a, b, preferred_element_type=jnp.float32, precision=lax.Precision.DEFAULT)


def low_part(x):
    return x - x.astype(jnp.bfloat16).astype(jnp.float32)


def down(table, x):
    return dot(table, jnp.concatenate([x, low_part(x), x], axis=0))


def joined(x):
    gap = jnp.zeros((PADDED // 2 - HALF, x[0].shape[1]), jnp.float32)
    return jnp.concatenate([x[0], gap, x[1], gap], axis=0)


def along(x, high, low):
    return dot(x, high) + dot(low_part(x), high) + dot(x, low)


def fill_tables(wide_ahead, wide_back, lane_ahead, lane_back, factors):
    rows = lax.broadcasted_iota(jnp.int32, (2 * N, 2 * LANES), 0)
    cols = lax.broadcasted_iota(jnp.int32, (2 * N, 2 * LANES), 1)
    for u in range(8):
        start = 2 * N * u % LANES
        move = jnp.where(cols == rows + start, 1.0, 0.0)
        for part in range(2):
            lane_ahead[u, part] = jnp.zeros((2 * LANES, 2 * LANES), jnp.float32)
            lane_ahead[u, part, start : start + 2 * N, :] = wide_ahead[part]
            lane_back[u, part] = dot(wide_back[part], move)

    def wave(i):
        f = jnp.where(i <= HALF, i, i - HALF)
        return (f * f).astype(jnp.float32), jnp.where((i == 0) | (i == HALF), 1.0, 2.0).astype(jnp.float32)

    factor = (2.0 * math.pi / (N * spacing)) ** 2
    square_b, weight_b = wave(lax.broadcasted_iota(jnp.int32, (N, LANES), 0))
    square_c, weight_c = wave(lax.broadcasted_iota(jnp.int32, (N, LANES), 1))
    inside = lax.broadcasted_iota(jnp.int32, (N, LANES), 1) < N

    def fill(i, _):
        square_a, weight_a = wave(i)
        ksq = factor * (square_a + square_b + square_c)
        keep = (ksq > 0) & inside
        coulomb = jnp.where(keep, 4.0 * math.pi / jnp.where(keep, ksq, 1.0), 0.0)
        factors[pl.ds(pl.multiple_of(i * N, 8), N), :] = coulomb * (weight_a * weight_b * weight_c) / float(N**3)
        return 0

    lax.fori_loop(0, N, fill, 0)


def exchange(homes, visit, home_outs, visit_out, first, tables, lane_ahead, lane_back, factors, u, w):
    ahead, back, half_ahead, half_back = tables
    pairs = len(homes)
    WIDE = 2 * LANES
    TAIL = PLANE // WIDE * WIDE
    body = 20 // pairs

    def flat_ahead(tiles):
        for at, width in tiles:
            for p in range(pairs):
                x = joined([homes[p][h, :, pl.ds(at, width)] * visit[h, :, pl.ds(at, width)] for h in range(2)])
                if width < LANES:
                    x = jnp.concatenate([x, jnp.zeros((PADDED, LANES - width), jnp.float32)], axis=1)
                u[p, :, pl.ds(at, max(width, LANES))] = down(half_ahead[...], x)

    def wide_tiles(i):
        return [(pl.multiple_of((i * body + k) * WIDE, LANES), WIDE) for k in range(body)]

    def loop(count, work, start=0):
        def step(i, _):
            work(i)
            return 0

        lax.fori_loop(start, count, step, 0)

    loop(TAIL // WIDE // body, lambda i: flat_ahead(wide_tiles(i)))
    flat_ahead([(TAIL, PLANE - TAIL)])

    def places_of(blocks):
        return [(p, t) for t in blocks for p in range(pairs)]

    def base(t):
        return pl.multiple_of(t * 9 * LANES, LANES)

    def line(t, k):
        return pl.multiple_of((t * 8 + k) * 2 * N, 8)

    def lines_ahead(blocks, count):
        for k in range(count):
            at = 2 * N * k // LANES * LANES
            x = jnp.concatenate([u[p, :, pl.ds(base(t) + at, WIDE)] for p, t in places_of(blocks)], axis=0)
            y = along(x, lane_ahead[k, 0], lane_ahead[k, 1])
            for i, (p, t) in enumerate(places_of(blocks)):
                for half in range(2):
                    part = y[N * i : N * (i + 1), LANES * half : LANES * (half + 1)]
                    w[p, pl.ds(line(t, k) + half * N, N), :] = part

    def block_range(i):
        return [i * 2 // pairs + j for j in range(2 // pairs)]

    loop(2 * pairs, lambda i: lines_ahead(block_range(i), 8))
    lines_ahead([4], 4)

    def at(i):
        return [(0, i), (1, i)] if pairs == 2 else [(0, 2 * i), (0, 2 * i + 1)]

    def load_w(i):
        return jnp.concatenate([w[p, pl.ds(q, N, stride=N), :] for p, q in at(i)], axis=1)

    def store_w(i, y):
        for half, (p, q) in enumerate(at(i)):
            w[p, pl.ds(q, N, stride=N), :] = y[:, LANES * half : LANES * (half + 1)]

    def ahead_b(i, x):
        y = down(ahead[...], x)
        return y * jnp.concatenate([factors[pl.ds(pl.multiple_of(q * N, 8), N), :] for _, q in at(i)], axis=1)

    def middle(i):
        now = [i * STRIP + k for k in range(STRIP)]
        before = [i * STRIP - STRIP + k for k in range(STRIP)]
        xs, ys = [load_w(q) for q in now], [load_w(q) for q in before]
        xs = [ahead_b(q, x) for q, x in zip(now, xs)]
        ys = [down(back[...], y) for y in ys]
        for q, x in zip(now, xs):
            store_w(q, x)
        for q, y in zip(before, ys):
            store_w(q, y)

    count = N * pairs // 2
    for q, x in [(q, ahead_b(q, load_w(q))) for q in range(STRIP)]:
        store_w(q, x)
    loop(count // STRIP, middle, 1)
    for q, y in [(q, down(back[...], load_w(q))) for q in range(count - STRIP, count)]:
        store_w(q, y)

    def lines_back(blocks, count):
        total = {}
        for k in range(count):
            tile = 2 * N * k // LANES
            x = jnp.concatenate(
                [
                    jnp.concatenate([w[p, pl.ds(line(t, k) + half * N, N), :] for half in range(2)], axis=1)
                    for p, t in places_of(blocks)
                ],
                axis=0,
            )
            y = along(x, lane_back[k, 0], lane_back[k, 1])
            for half in range(2):
                part = y[:, LANES * half : LANES * (half + 1)]
                total[tile + half] = total[tile + half] + part if tile + half in total else part
        for tile, value in total.items():
            for i, (p, t) in enumerate(places_of(blocks)):
                u[p, :, pl.ds(base(t) + tile * LANES, LANES)] = value[N * i : N * (i + 1)]

    loop(2 * pairs, lambda i: lines_back(block_range(i), 8))
    lines_back([4], 4)

    def flat_back(tiles):
        for at, width in tiles:
            cells = pl.ds(at, width)
            total = [0.0 if first[1] else visit_out[h, :, cells] for h in range(2)]
            for p in range(pairs):
                v = down(half_back[...], u[p, :, pl.ds(at, max(width, LANES))])[:, :width]
                for h in range(2):
                    part = v[PADDED // 2 * h : PADDED // 2 * h + HALF]
                    mine = part * visit[h, :, cells]
                    home_outs[p][h, :, cells] = -mine if first[0] else home_outs[p][h, :, cells] - mine
                    total[h] = total[h] - part * homes[p][h, :, cells]
            for h in range(2):
                visit_out[h, :, cells] = total[h]

    loop(TAIL // WIDE // body, lambda i: flat_back(wide_tiles(i)))
    flat_back([(TAIL, PLANE - TAIL)])


HBM = pl.BlockSpec(memory_space=pl.ANY)
VMEM = pl.BlockSpec(memory_space=pltpu.VMEM)


def places():
    n, g, count = lax.axis_index("band"), lax.axis_index("grid"), lax.axis_size("band")
    core, r = lax.rem(n, 2), lax.rem(n, 4)
    swap = (n, 1 - g)
    x_to = (lax.rem(n + 2, count), 1 - g)
    x_from = (jnp.where(r == 1, n + 1, lax.rem(n + count - 2, count)), 1 - g)
    r_to = (lax.rem(n + count - 1, count), 1 - g)
    y_to, y_from = (lax.rem(n + 1 + 2 * core, count), g), (lax.rem(n + count - 3 + 2 * core, count), g)
    side = (n + 1 - 2 * core, g)
    return g, r, swap, x_to, x_from, r_to, y_to, y_from, side


def meet(senders, count):
    barrier = pltpu.get_barrier_semaphore()
    for use, device in senders:

        def signal():
            pl.semaphore_signal(barrier, inc=1, device_id=device, device_id_type=MESH)

        signal() if use is None else pl.when(use)(signal)
    pl.semaphore_wait(barrier, count)


def sender(send, recv):
    index = iter(range(64))

    def make(src, dst, device, into=None):
        i = next(index)
        j = i if into is None else into
        copy = pltpu.make_async_remote_copy(src, dst, send.at[i], recv.at[j], device_id=device, device_id_type=MESH)
        return copy, i

    return make


def exchange_kernel(
    bands, ahead, back, half_ahead, half_back, wide_ahead, wide_back, out,
    flat, outs, lane_ahead, lane_back, factors, u, w, from_s, from_x, from_y, from_r, from_e, send, recv, local,
):
    g, r, swap, x_to, x_from, r_to, y_to, y_from, side = places()
    sends_x, relays = r != 3, r == 2
    f = 1 - g
    pieces = range(len(CHUNKS))
    make = sender(send, recv)

    def cells(c):
        return pl.ds(*CHUNKS[c])

    def many(src, dst, device, into=None):
        made = [
            make(src.at[:, cells(c)], dst.at[:, cells(c)], device, None if into is None else into[c]) for c in pieces
        ]
        return [copy for copy, _ in made], [i for _, i in made]

    meet(
        [(None, swap), (None, x_from), (None, y_from), (None, side)],
        3 + jnp.where(sends_x, 1, 0) + jnp.where(relays, 1, 0),
    )
    e1, _ = many(bands.at[g], flat.at[g, g], swap)
    x1, x1_at = make(bands.at[f], flat.at[2, g], x_to)
    y1, _ = make(bands.at[f], flat.at[4, g], y_to)
    e2, _ = make(bands.at[f], flat.at[f, g], swap)
    x2, x2_at = many(flat.at[f, f], flat.at[2, f], x_to)
    y2, _ = many(flat.at[f, f], flat.at[4, f], y_to)
    s1, _ = make(flat.at[2, f], flat.at[3, f], side)
    s2, _ = many(flat.at[2, g], flat.at[3, g], side)
    r1, _ = make(flat.at[4, g], flat.at[2, g], r_to, x1_at)
    r2, _ = many(flat.at[4, f], flat.at[2, f], r_to, x2_at)
    loads = [pltpu.make_async_copy(bands.at[b], flat.at[b, g], local.at[b]) for b in range(2)]
    for copy in e1:
        copy.start()

    @pl.when(sends_x)
    def _():
        x1.start()

    y1.start()
    for copy in loads:
        copy.start()
    fill_tables(wide_ahead, wide_back, lane_ahead, lane_back, factors)
    for c in pieces:
        e1[c].wait_recv()

        @pl.when(sends_x)
        def _():
            x2[c].start()

        y2[c].start()
    e2.start()

    def pairs(homes, slot, first):
        exchange(
            [flat.at[b] for b in homes], flat.at[slot], [outs.at[b] for b in homes], outs.at[slot], first,
            (ahead, back, half_ahead, half_back), lane_ahead, lane_back, factors, u, w,
        )

    s_back = [many(outs.at[3, h], from_s.at[h], side)[0] for h in (g, f)]
    y_back = [many(outs.at[4, h], from_y.at[h], y_from)[0] for h in (f, g)]
    x_back = [many(outs.at[2, h], from_x.at[h], x_from)[0] for h in (g, f)]
    r_back = [many(outs.at[2, h], from_r.at[h], x_from)[0] for h in (g, f)]
    e1_back, _ = make(outs.at[g, f], from_e.at[g], swap)
    e2_back, _ = many(outs.at[f, f], from_e.at[f], swap)

    y1.wait_recv()

    @pl.when(relays)
    def _():
        r1.start()

    for c in pieces:
        y2[c].wait_recv()

        @pl.when(relays)
        def _():
            r2[c].start()

    for copy in loads:
        copy.wait()
    pairs([f], 4, (True, True))
    e2.wait_recv()
    pairs([g], 4, (True, False))

    @pl.when(r != 2)
    def _():
        for copy in y_back[0] + y_back[1]:
            copy.start()

    x1.wait_recv()
    s1.start()
    for c in pieces:
        x2[c].wait_recv()
        s2[c].start()
    pairs([0, 1], 2, (False, True))
    s1.wait_recv()
    for copy in s2:
        copy.wait_recv()
    pairs([0, 1], 3, (False, True))
    for copy in s_back[0] + s_back[1]:
        copy.start()
    e1_back.start()
    for k, h in enumerate((g, f)):
        for c in pieces:
            s_back[k][c].wait_recv()
            outs[2, h, :, cells(c)] += from_s[h, :, cells(c)]

            @pl.when(r != 1)
            def _():
                x_back[k][c].start()

            @pl.when(r == 1)
            def _():
                r_back[k][c].start()

    @pl.when(relays)
    def _():
        for k, h in enumerate((f, g)):
            for c in pieces:
                r_back[k][c].wait_recv()
                outs[4, h, :, cells(c)] += from_r[h, :, cells(c)]
                y_back[k][c].start()

    for k, h in enumerate((f, g)):
        for c in pieces:

            @pl.when(sends_x)
            def _():
                x_back[k][c].wait_recv()
                outs[f, h, :, cells(c)] += from_x[h, :, cells(c)]

            y_back[k][c].wait_recv()
            outs[f, h, :, cells(c)] += from_y[h, :, cells(c)]
            if k == 0:
                e2_back[c].start()
    e1_back.wait_recv()
    outs[f, g] += from_e[f]
    stores = [pltpu.make_async_copy(outs.at[b, g], out.at[b], local.at[i]) for i, b in enumerate((f, g))]
    stores[0].start()
    for c in pieces:
        e2_back[c].wait_recv()
        outs[g, g, :, cells(c)] += from_e[g, :, cells(c)]
    stores[1].start()
    for copy in stores:
        copy.wait()
    for copy in e1 + [y1, e2] + y2 + [s1] + s2 + s_back[0] + s_back[1] + y_back[0] + y_back[1] + [e1_back] + e2_back:
        copy.wait_send()

    @pl.when(sends_x)
    def _():
        for copy in [x1] + x2:
            copy.wait_send()

    @pl.when(relays)
    def _():
        for copy in [r1] + r2:
            copy.wait_send()

    @pl.when(r != 1)
    def _():
        for copy in x_back[0] + x_back[1]:
            copy.wait_send()

    @pl.when(r == 1)
    def _():
        for copy in r_back[0] + r_back[1]:
            copy.wait_send()


def local(bands):
    band = pltpu.VMEM((2, HALF, PLANE), jnp.float32)
    table = pltpu.VMEM((8, 2, 2 * LANES, 2 * LANES), jnp.float32)
    return pl.pallas_call(
        exchange_kernel,
        out_shape=jax.ShapeDtypeStruct((2, HALF, PLANE), jnp.float32),
        in_specs=[HBM] + [VMEM] * 6,
        out_specs=HBM,
        scratch_shapes=[
            pltpu.VMEM((5, 2, HALF, PLANE), jnp.float32),
            pltpu.VMEM((5, 2, HALF, PLANE), jnp.float32),
            table, table,
            pltpu.VMEM((ROWS, LANES), jnp.float32),
            pltpu.VMEM((2, N, 41 * LANES), jnp.float32),
            pltpu.VMEM((2, ROWS, LANES), jnp.float32),
            band, band, band, band, band,
            pltpu.SemaphoreType.DMA((48,)), pltpu.SemaphoreType.DMA((48,)), pltpu.SemaphoreType.DMA((2,)),
        ],
        compiler_params=pltpu.CompilerParams(collective_id=0, has_side_effects=True, vmem_limit_bytes=63 * 1024 * 1024),
        name="exchange_terms",
    )(bands, *constants())


def solution(mesh):
    return jax.shard_map(
        local,
        mesh=mesh,
        in_specs=(P("band", "grid", None),),
        out_specs=P("band", "grid", None),
        check_vma=False,
    )
```

```python
import functools
import math

import jax
import jax.numpy as jnp
import numpy as np
from jax import lax
from jax.experimental import pallas as pl
from jax.experimental.pallas import tpu as pltpu
from jax.sharding import PartitionSpec as P

N = 72
HALF = 36
LANES = 128
ROWS = N * N
PLANE = N * N
MESH = pl.DeviceIdType.MESH
LINE = 41 * LANES
FOLD = 20 * LANES
LAST = 4 * LINE
LENGTH = LAST + LINE - FOLD
CHUNKS = ((0, 62 * LANES), (62 * LANES, 62 * LANES), (124 * LANES, 61 * LANES))
STRIP = 12
spacing = 0.5167


def rounded(x):
    return x.astype(jnp.bfloat16).astype(np.float32)


def constants():
    index = np.arange(N)
    freq = np.where(index <= HALF, index, index - HALF)
    phase = (freq[:, None] * index[None, :] % N) * (2.0 * math.pi / N)
    table = np.where(index[:, None] <= HALF, np.cos(phase), np.sin(phase)).astype(np.float32)

    def stacked(t):
        return np.concatenate([t, t, t - rounded(t)], axis=1)

    def blocks(m):
        wide = np.zeros((2 * N, 2 * LANES), np.float32)
        wide[:N, :N] = m
        wide[N:, LANES : LANES + N] = m
        return np.stack([rounded(wide), rounded(wide - rounded(wide))])

    halved = np.zeros((2, N, 80), np.float32)
    for fold in range(2):
        for row in range(N):
            half, r = divmod(row, HALF)
            halved[fold, :, 40 * half + r + (4 * fold if r >= 32 else 0)] = table[:, row]
    half_ahead = np.stack([stacked(m) for m in halved])
    half_back = np.stack([stacked(m.T) for m in halved])
    return stacked(table), stacked(table.T), half_ahead, half_back, blocks(table.T), blocks(table.T).transpose(0, 2, 1)


def dot(a, b):
    return jnp.dot(a, b, preferred_element_type=jnp.float32, precision=lax.Precision.DEFAULT)


def low_part(x):
    return x - x.astype(jnp.bfloat16).astype(jnp.float32)


def down(table, x):
    return dot(table, jnp.concatenate([x, low_part(x), x], axis=0))


def lanes_of(fold, at, width):
    return [pl.ds(LINE * i + at, width) for i in range(4)] + [pl.ds(LAST + at - FOLD * fold, width)]


def along(x, high, low):
    return dot(x, high) + dot(low_part(x), high) + dot(x, low)


def fill_tables(wide_ahead, wide_back, lane_ahead, lane_back, factors):
    rows = lax.broadcasted_iota(jnp.int32, (2 * N, 2 * LANES), 0)
    cols = lax.broadcasted_iota(jnp.int32, (2 * N, 2 * LANES), 1)
    for u in range(8):
        start = 2 * N * u % LANES
        move = jnp.where(cols == rows + start, 1.0, 0.0)
        for part in range(2):
            lane_ahead[u, part] = jnp.zeros((2 * LANES, 2 * LANES), jnp.float32)
            lane_ahead[u, part, start : start + 2 * N, :] = wide_ahead[part]
            lane_back[u, part] = dot(wide_back[part], move)

    def wave(i):
        f = jnp.where(i <= HALF, i, i - HALF)
        return (f * f).astype(jnp.float32), jnp.where((i == 0) | (i == HALF), 1.0, 2.0).astype(jnp.float32)

    factor = (2.0 * math.pi / (N * spacing)) ** 2
    square_b, weight_b = wave(lax.broadcasted_iota(jnp.int32, (N, LANES), 0))
    square_c, weight_c = wave(lax.broadcasted_iota(jnp.int32, (N, LANES), 1))
    inside = lax.broadcasted_iota(jnp.int32, (N, LANES), 1) < N

    def fill(i, _):
        square_a, weight_a = wave(i)
        ksq = factor * (square_a + square_b + square_c)
        keep = (ksq > 0) & inside
        coulomb = jnp.where(keep, 4.0 * math.pi / jnp.where(keep, ksq, 1.0), 0.0)
        factors[pl.ds(pl.multiple_of(i * N, 8), N), :] = coulomb * (weight_a * weight_b * weight_c) / float(N**3)
        return 0

    lax.fori_loop(0, N, fill, 0)


def exchange(homes, visit, home_outs, visit_out, first, tables, lane_ahead, lane_back, factors, u, w):
    ahead, back, half_ahead, half_back = tables
    pairs = len(homes)
    WIDE = 2 * LANES
    TAIL = PLANE // WIDE * WIDE
    body = 20 // pairs

    def flat_ahead(tiles):
        for fold, at, width in tiles:
            where = lanes_of(fold, at, width)
            for p in range(pairs):
                x = [homes[p][h, :, lanes] * visit[h, :, lanes] for h in range(2) for lanes in where]
                u[p, :, pl.ds(at, width)] = down(half_ahead[fold], jnp.concatenate(x, axis=0))

    def wide_tiles(i):
        if pairs == 1:
            return [(k // 10, k * WIDE, WIDE) for k in range(body)]
        return [(i, pl.multiple_of((i * body + k) * WIDE, LANES), WIDE) for k in range(body)]

    def loop(count, work, start=0):
        def step(i, _):
            work(i)
            return 0

        lax.fori_loop(start, count, step, 0)

    loop(TAIL // WIDE // body, lambda i: flat_ahead(wide_tiles(i)))
    flat_ahead([(1, TAIL, LANES)])

    def places_of(blocks):
        return [(p, t) for t in blocks for p in range(pairs)]

    def base(t):
        return pl.multiple_of(t * 9 * LANES, LANES)

    def line(t, k):
        return pl.multiple_of((t * 8 + k) * 2 * N, 8)

    def lines_ahead(blocks, count):
        for k in range(count):
            at = 2 * N * k // LANES * LANES
            x = jnp.concatenate([u[p, :, pl.ds(base(t) + at, WIDE)] for p, t in places_of(blocks)], axis=0)
            y = along(x, lane_ahead[k, 0], lane_ahead[k, 1])
            for i, (p, t) in enumerate(places_of(blocks)):
                for half in range(2):
                    part = y[N * i : N * (i + 1), LANES * half : LANES * (half + 1)]
                    w[p, pl.ds(line(t, k) + half * N, N), :] = part

    def block_range(i):
        return [i * 2 // pairs + j for j in range(2 // pairs)]

    loop(2 * pairs, lambda i: lines_ahead(block_range(i), 8))
    lines_ahead([4], 4)

    def at(i):
        return [(0, i), (1, i)] if pairs == 2 else [(0, 2 * i), (0, 2 * i + 1)]

    def load_w(i):
        return jnp.concatenate([w[p, pl.ds(q, N, stride=N), :] for p, q in at(i)], axis=1)

    def store_w(i, y):
        for half, (p, q) in enumerate(at(i)):
            w[p, pl.ds(q, N, stride=N), :] = y[:, LANES * half : LANES * (half + 1)]

    def ahead_b(i, x):
        y = down(ahead[...], x)
        return y * jnp.concatenate([factors[pl.ds(pl.multiple_of(q * N, 8), N), :] for _, q in at(i)], axis=1)

    def middle(i):
        now = [i * STRIP + k for k in range(STRIP)]
        before = [i * STRIP - STRIP + k for k in range(STRIP)]
        xs, ys = [load_w(q) for q in now], [load_w(q) for q in before]
        xs = [ahead_b(q, x) for q, x in zip(now, xs)]
        ys = [down(back[...], y) for y in ys]
        for q, x in zip(now, xs):
            store_w(q, x)
        for q, y in zip(before, ys):
            store_w(q, y)

    count = N * pairs // 2
    for q, x in [(q, ahead_b(q, load_w(q))) for q in range(STRIP)]:
        store_w(q, x)
    loop(count // STRIP, middle, 1)
    for q, y in [(q, down(back[...], load_w(q))) for q in range(count - STRIP, count)]:
        store_w(q, y)

    def lines_back(blocks, count):
        total = {}
        for k in range(count):
            tile = 2 * N * k // LANES
            x = jnp.concatenate(
                [
                    jnp.concatenate([w[p, pl.ds(line(t, k) + half * N, N), :] for half in range(2)], axis=1)
                    for p, t in places_of(blocks)
                ],
                axis=0,
            )
            y = along(x, lane_back[k, 0], lane_back[k, 1])
            for half in range(2):
                part = y[:, LANES * half : LANES * (half + 1)]
                total[tile + half] = total[tile + half] + part if tile + half in total else part
        for tile, value in total.items():
            for i, (p, t) in enumerate(places_of(blocks)):
                u[p, :, pl.ds(base(t) + tile * LANES, LANES)] = value[N * i : N * (i + 1)]

    loop(2 * pairs, lambda i: lines_back(block_range(i), 8))
    lines_back([4], 4)

    last = pl.ds(LAST, LENGTH - LAST)
    for out, new in list(zip(home_outs, first[0])) + [(visit_out, first[1])]:
        if new:
            for h in range(2):
                out[h, :, last] = jnp.zeros((8, LENGTH - LAST), jnp.float32)

    def flat_back(tiles):
        for fold, at, width in tiles:
            vs = [down(half_back[fold], u[p, :, pl.ds(at, width)]) for p in range(pairs)]
            for h in range(2):
                for i, lanes in enumerate(lanes_of(fold, at, width)):
                    total = visit_out[h, :, lanes] if i == 4 or not first[1] else 0.0
                    other = visit[h, :, lanes]
                    for p in range(pairs):
                        part = vs[p][40 * h + 8 * i : 40 * h + 8 * (i + 1)]
                        before = home_outs[p][h, :, lanes] if i == 4 or not first[0][p] else 0.0
                        home_outs[p][h, :, lanes] = before - part * other
                        total = total - part * homes[p][h, :, lanes]
                    visit_out[h, :, lanes] = total

    loop(TAIL // WIDE // body, lambda i: flat_back(wide_tiles(i)))
    flat_back([(1, TAIL, LANES)])


HBM = pl.BlockSpec(memory_space=pl.ANY)
VMEM = pl.BlockSpec(memory_space=pltpu.VMEM)


def places():
    n, g, count = lax.axis_index("band"), lax.axis_index("grid"), lax.axis_size("band")
    core, r = lax.rem(n, 2), lax.rem(n, 4)
    swap = (n, 1 - g)
    x_to = (lax.rem(n + 2, count), 1 - g)
    x_from = (jnp.where(r == 1, n + 1, lax.rem(n + count - 2, count)), 1 - g)
    r_to = (lax.rem(n + count - 1, count), 1 - g)
    y_to, y_from = (lax.rem(n + 1 + 2 * core, count), g), (lax.rem(n + count - 3 + 2 * core, count), g)
    side = (n + 1 - 2 * core, g)
    return g, r, swap, x_to, x_from, r_to, y_to, y_from, side


def meet(senders, count):
    barrier = pltpu.get_barrier_semaphore()
    for use, device in senders:

        def signal():
            pl.semaphore_signal(barrier, inc=1, device_id=device, device_id_type=MESH)

        signal() if use is None else pl.when(use)(signal)
    pl.semaphore_wait(barrier, count)


def sender(send, recv):
    index = iter(range(64))

    def make(src, dst, device, into=None):
        i = next(index)
        j = i if into is None else into
        copy = pltpu.make_async_remote_copy(src, dst, send.at[i], recv.at[j], device_id=device, device_id_type=MESH)
        return copy, i

    return make


def exchange_kernel(
    bands, ahead, back, half_ahead, half_back, wide_ahead, wide_back, out,
    flat, outs, lane_ahead, lane_back, factors, u, w, from_s, from_x, from_y, from_r, from_e, send, recv, local,
):
    g, r, swap, x_to, x_from, r_to, y_to, y_from, side = places()
    sends_x, relays = r != 3, r == 2
    f = 1 - g
    pieces = range(len(CHUNKS))
    make = sender(send, recv)

    def cells(c):
        return pl.ds(*CHUNKS[c])

    def many(src, dst, device, into=None):
        made = [
            make(src.at[:, cells(c)], dst.at[:, cells(c)], device, None if into is None else into[c]) for c in pieces
        ]
        return [copy for copy, _ in made], [i for _, i in made]

    meet(
        [(None, swap), (None, x_from), (None, y_from), (None, side)],
        3 + jnp.where(sends_x, 1, 0) + jnp.where(relays, 1, 0),
    )
    e1, _ = many(bands.at[g], flat.at[g, g], swap)
    x1, x1_at = make(bands.at[f], flat.at[2, g], x_to)
    y1, _ = make(bands.at[f], flat.at[4, g], y_to)
    e2, _ = make(bands.at[f], flat.at[f, g], swap)
    x2, x2_at = many(flat.at[f, f], flat.at[2, f], x_to)
    y2, _ = many(flat.at[f, f], flat.at[4, f], y_to)
    s1, _ = make(flat.at[2, f], flat.at[3, f], side)
    s2, _ = many(flat.at[2, g], flat.at[3, g], side)
    r1, _ = make(flat.at[4, g], flat.at[2, g], r_to, x1_at)
    r2, _ = many(flat.at[4, f], flat.at[2, f], r_to, x2_at)
    loads = [pltpu.make_async_copy(bands.at[b], flat.at[b, g], local.at[b]) for b in range(2)]
    for copy in e1:
        copy.start()

    @pl.when(sends_x)
    def _():
        x1.start()

    y1.start()
    for copy in loads:
        copy.start()
    fill_tables(wide_ahead, wide_back, lane_ahead, lane_back, factors)
    for c in pieces:
        e1[c].wait_recv()

        @pl.when(sends_x)
        def _():
            x2[c].start()

        y2[c].start()
    e2.start()

    def pairs(homes, slot, first):
        exchange(
            [flat.at[b] for b in homes], flat.at[slot], [outs.at[b] for b in homes], outs.at[slot], first,
            (ahead, back, half_ahead, half_back), lane_ahead, lane_back, factors, u, w,
        )

    s_back = [many(outs.at[3, h], from_s.at[h], side)[0] for h in (g, f)]
    y_back = [many(outs.at[4, h], from_y.at[h], y_from)[0] for h in (f, g)]
    x_back = [many(outs.at[2, h], from_x.at[h], x_from)[0] for h in (g, f)]
    r_back = [many(outs.at[2, h], from_r.at[h], x_from)[0] for h in (g, f)]
    e1_back, _ = make(outs.at[g, f], from_e.at[g], swap)
    e2_back, _ = many(outs.at[f, f], from_e.at[f], swap)

    y1.wait_recv()

    @pl.when(relays)
    def _():
        r1.start()

    for c in pieces:
        y2[c].wait_recv()

        @pl.when(relays)
        def _():
            r2[c].start()

    for copy in loads:
        copy.wait()
    pairs([f], 4, ((True,), True))
    e2.wait_recv()
    x1.wait_recv()
    s1.start()
    for c in pieces:
        x2[c].wait_recv()
        s2[c].start()
    pairs([f, g], 2, ((False, True), True))
    s1.wait_recv()
    for copy in s2:
        copy.wait_recv()
    pairs([f, g], 3, ((False, False), True))
    for copy in s_back[0] + s_back[1]:
        copy.start()
    for k, h in enumerate((g, f)):
        for c in pieces:
            s_back[k][c].wait_recv()
            outs[2, h, :, cells(c)] += from_s[h, :, cells(c)]

            @pl.when(r != 1)
            def _():
                x_back[k][c].start()

            @pl.when(r == 1)
            def _():
                r_back[k][c].start()

    pairs([g], 4, ((False,), False))
    e1_back.start()

    @pl.when(r != 2)
    def _():
        for copy in y_back[0] + y_back[1]:
            copy.start()

    for k, h in enumerate((f, g)):
        for c in pieces:

            @pl.when(relays)
            def _():
                r_back[k][c].wait_recv()
                outs[4, h, :, cells(c)] += from_r[h, :, cells(c)]
                y_back[k][c].start()

            @pl.when(sends_x)
            def _():
                x_back[k][c].wait_recv()
                outs[f, h, :, cells(c)] += from_x[h, :, cells(c)]

            y_back[k][c].wait_recv()
            outs[f, h, :, cells(c)] += from_y[h, :, cells(c)]
            if k == 0:
                e2_back[c].start()
    e1_back.wait_recv()
    outs[f, g] += from_e[f]
    stores = [pltpu.make_async_copy(outs.at[b, g], out.at[b], local.at[i]) for i, b in enumerate((f, g))]
    stores[0].start()
    for c in pieces:
        e2_back[c].wait_recv()
        outs[g, g, :, cells(c)] += from_e[g, :, cells(c)]
    stores[1].start()
    for copy in stores:
        copy.wait()
    for copy in e1 + [y1, e2] + y2 + [s1] + s2 + s_back[0] + s_back[1] + y_back[0] + y_back[1] + [e1_back] + e2_back:
        copy.wait_send()

    @pl.when(sends_x)
    def _():
        for copy in [x1] + x2:
            copy.wait_send()

    @pl.when(relays)
    def _():
        for copy in [r1] + r2:
            copy.wait_send()

    @pl.when(r != 1)
    def _():
        for copy in x_back[0] + x_back[1]:
            copy.wait_send()

    @pl.when(r == 1)
    def _():
        for copy in r_back[0] + r_back[1]:
            copy.wait_send()


def blocked(bands):
    x = jnp.pad(bands, ((0, 0), (0, 0), (0, LINE - PLANE)))
    last = jnp.pad(x[:, 32:, :FOLD], ((0, 0), (0, 0), (0, LINE - 2 * FOLD)))
    parts = [x[:, 8 * i : 8 * (i + 1)] for i in range(4)] + [jnp.concatenate([last, x[:, 32:, FOLD:]], axis=1)]
    return jnp.concatenate(parts, axis=2)


def unblocked(x):
    last = jnp.concatenate([x[:, :4, LAST : LAST + FOLD], x[:, 4:, LAST : LAST + PLANE - FOLD]], axis=2)
    return jnp.concatenate([x[:, :, LINE * i : LINE * i + PLANE] for i in range(4)] + [last], axis=1)


def local(bands):
    band = pltpu.VMEM((2, 8, LENGTH), jnp.float32)
    five = pltpu.VMEM((5, 2, 8, LENGTH), jnp.float32)
    table = pltpu.VMEM((8, 2, 2 * LANES, 2 * LANES), jnp.float32)
    terms = pl.pallas_call(
        exchange_kernel,
        out_shape=jax.ShapeDtypeStruct((2, 8, LENGTH), jnp.float32),
        in_specs=[HBM] + [VMEM] * 6,
        out_specs=HBM,
        scratch_shapes=[
            five, five, table, table,
            pltpu.VMEM((ROWS, LANES), jnp.float32),
            pltpu.VMEM((2, N, LINE), jnp.float32),
            pltpu.VMEM((2, ROWS, LANES), jnp.float32),
            band, band, band, band, band,
            pltpu.SemaphoreType.DMA((48,)), pltpu.SemaphoreType.DMA((48,)), pltpu.SemaphoreType.DMA((2,)),
        ],
        compiler_params=pltpu.CompilerParams(collective_id=0, has_side_effects=True, vmem_limit_bytes=63 * 1024 * 1024),
        name="exchange_terms",
    )(blocked(bands), *constants())
    return unblocked(terms)


def solution(mesh):
    return jax.shard_map(
        local,
        mesh=mesh,
        in_specs=(P("band", "grid", None),),
        out_specs=P("band", "grid", None),
        check_vma=False,
    )
```

```python
import functools
import math

import jax
import jax.numpy as jnp
import numpy as np
from jax import lax
from jax.experimental import pallas as pl
from jax.experimental.pallas import tpu as pltpu
from jax.sharding import PartitionSpec as P

N = 72
HALF = 36
LANES = 128
ROWS = N * N
PLANE = N * N
MESH = pl.DeviceIdType.MESH
LINE = 41 * LANES
FOLD = 20 * LANES
LAST = 4 * LINE
LENGTH = LAST + LINE - FOLD
CHUNKS = ((0, 62 * LANES), (62 * LANES, 62 * LANES), (124 * LANES, 61 * LANES))
STRIP = 12
spacing = 0.5167


def rounded(x):
    return x.astype(jnp.bfloat16).astype(np.float32)


def constants():
    index = np.arange(N)
    freq = np.where(index <= HALF, index, index - HALF)
    phase = (freq[:, None] * index[None, :] % N) * (2.0 * math.pi / N)
    table = np.where(index[:, None] <= HALF, np.cos(phase), np.sin(phase)).astype(np.float32)

    def stacked(t):
        return np.concatenate([t, t, t - rounded(t)], axis=1)

    def blocks(m):
        wide = np.zeros((2 * N, 2 * LANES), np.float32)
        wide[:N, :N] = m
        wide[N:, LANES : LANES + N] = m
        return np.stack([rounded(wide), rounded(wide - rounded(wide))])

    halved = np.zeros((2, N, 80), np.float32)
    for fold in range(2):
        for row in range(N):
            half, r = divmod(row, HALF)
            halved[fold, :, 40 * half + r + (4 * fold if r >= 32 else 0)] = table[:, row]
    half_ahead = np.stack([stacked(m) for m in halved])
    half_back = np.stack([stacked(m.T) for m in halved])
    return stacked(table), stacked(table.T), half_ahead, half_back, blocks(table.T), blocks(table.T).transpose(0, 2, 1)


def dot(a, b):
    return jnp.dot(a, b, preferred_element_type=jnp.float32, precision=lax.Precision.DEFAULT)


def low_part(x):
    return x - x.astype(jnp.bfloat16).astype(jnp.float32)


def down(table, x):
    return dot(table, jnp.concatenate([x, low_part(x), x], axis=0))


def lanes_of(fold, at, width):
    return [pl.ds(LINE * i + at, width) for i in range(4)] + [pl.ds(LAST + at - FOLD * fold, width)]


def along(x, high, low):
    return dot(x, high) + dot(low_part(x), high) + dot(x, low)


def fill_tables(wide_ahead, wide_back, lane_ahead, lane_back, factors):
    rows = lax.broadcasted_iota(jnp.int32, (2 * N, 2 * LANES), 0)
    cols = lax.broadcasted_iota(jnp.int32, (2 * N, 2 * LANES), 1)
    for u in range(8):
        start = 2 * N * u % LANES
        move = jnp.where(cols == rows + start, 1.0, 0.0)
        for part in range(2):
            lane_ahead[u, part] = jnp.zeros((2 * LANES, 2 * LANES), jnp.float32)
            lane_ahead[u, part, start : start + 2 * N, :] = wide_ahead[part]
            lane_back[u, part] = dot(wide_back[part], move)

    def wave(i):
        f = jnp.where(i <= HALF, i, i - HALF)
        return (f * f).astype(jnp.float32), jnp.where((i == 0) | (i == HALF), 1.0, 2.0).astype(jnp.float32)

    factor = (2.0 * math.pi / (N * spacing)) ** 2
    square_b, weight_b = wave(lax.broadcasted_iota(jnp.int32, (N, LANES), 0))
    square_c, weight_c = wave(lax.broadcasted_iota(jnp.int32, (N, LANES), 1))
    inside = lax.broadcasted_iota(jnp.int32, (N, LANES), 1) < N

    def fill(i, _):
        square_a, weight_a = wave(i)
        ksq = factor * (square_a + square_b + square_c)
        keep = (ksq > 0) & inside
        coulomb = jnp.where(keep, 4.0 * math.pi / jnp.where(keep, ksq, 1.0), 0.0)
        factors[pl.ds(pl.multiple_of(i * N, 8), N), :] = coulomb * (weight_a * weight_b * weight_c) / float(N**3)
        return 0

    lax.fori_loop(0, N, fill, 0)


def exchange(homes, visit, home_outs, visit_out, first, tables, lane_ahead, lane_back, factors, u, w):
    ahead, back, half_ahead, half_back = tables
    pairs = len(homes)
    WIDE = 2 * LANES
    TAIL = PLANE // WIDE * WIDE
    body = 20 // pairs

    def flat_ahead(tiles):
        for fold, at, width in tiles:
            where = lanes_of(fold, at, width)
            for p in range(pairs):
                x = [homes[p][h, :, lanes] * visit[h, :, lanes] for h in range(2) for lanes in where]
                u[p, :, pl.ds(at, width)] = down(half_ahead[fold], jnp.concatenate(x, axis=0))

    def wide_tiles(i):
        if pairs == 1:
            return [(k // 10, k * WIDE, WIDE) for k in range(body)]
        return [(i, pl.multiple_of((i * body + k) * WIDE, LANES), WIDE) for k in range(body)]

    def loop(count, work, start=0):
        def step(i, _):
            work(i)
            return 0

        lax.fori_loop(start, count, step, 0)

    loop(TAIL // WIDE // body, lambda i: flat_ahead(wide_tiles(i)))
    flat_ahead([(1, TAIL, LANES)])

    def places_of(blocks):
        return [(p, t) for t in blocks for p in range(pairs)]

    def base(t):
        return pl.multiple_of(t * 9 * LANES, LANES)

    def line(t, k):
        return pl.multiple_of((t * 8 + k) * 2 * N, 8)

    def lines_ahead(blocks, count):
        for k in range(count):
            at = 2 * N * k // LANES * LANES
            x = jnp.concatenate([u[p, :, pl.ds(base(t) + at, WIDE)] for p, t in places_of(blocks)], axis=0)
            y = along(x, lane_ahead[k, 0], lane_ahead[k, 1])
            for i, (p, t) in enumerate(places_of(blocks)):
                for half in range(2):
                    part = y[N * i : N * (i + 1), LANES * half : LANES * (half + 1)]
                    w[p, pl.ds(line(t, k) + half * N, N), :] = part

    def block_range(i):
        return [i * 2 // pairs + j for j in range(2 // pairs)]

    loop(2 * pairs, lambda i: lines_ahead(block_range(i), 8))
    lines_ahead([4], 4)

    def at(i):
        return [(0, i), (1, i)] if pairs == 2 else [(0, 2 * i), (0, 2 * i + 1)]

    def load_w(i):
        return jnp.concatenate([w[p, pl.ds(q, N, stride=N), :] for p, q in at(i)], axis=1)

    def store_w(i, y):
        for half, (p, q) in enumerate(at(i)):
            w[p, pl.ds(q, N, stride=N), :] = y[:, LANES * half : LANES * (half + 1)]

    def ahead_b(i, x):
        y = down(ahead[...], x)
        return y * jnp.concatenate([factors[pl.ds(pl.multiple_of(q * N, 8), N), :] for _, q in at(i)], axis=1)

    def middle(i):
        now = [i * STRIP + k for k in range(STRIP)]
        before = [i * STRIP - STRIP + k for k in range(STRIP)]
        xs, ys = [load_w(q) for q in now], [load_w(q) for q in before]
        xs = [ahead_b(q, x) for q, x in zip(now, xs)]
        ys = [down(back[...], y) for y in ys]
        for q, x in zip(now, xs):
            store_w(q, x)
        for q, y in zip(before, ys):
            store_w(q, y)

    count = N * pairs // 2
    for q, x in [(q, ahead_b(q, load_w(q))) for q in range(STRIP)]:
        store_w(q, x)
    loop(count // STRIP, middle, 1)
    for q, y in [(q, down(back[...], load_w(q))) for q in range(count - STRIP, count)]:
        store_w(q, y)

    def lines_back(blocks, count):
        total = {}
        for k in range(count):
            tile = 2 * N * k // LANES
            x = jnp.concatenate(
                [
                    jnp.concatenate([w[p, pl.ds(line(t, k) + half * N, N), :] for half in range(2)], axis=1)
                    for p, t in places_of(blocks)
                ],
                axis=0,
            )
            y = along(x, lane_back[k, 0], lane_back[k, 1])
            for half in range(2):
                part = y[:, LANES * half : LANES * (half + 1)]
                total[tile + half] = total[tile + half] + part if tile + half in total else part
        for tile, value in total.items():
            for i, (p, t) in enumerate(places_of(blocks)):
                u[p, :, pl.ds(base(t) + tile * LANES, LANES)] = value[N * i : N * (i + 1)]

    loop(2 * pairs, lambda i: lines_back(block_range(i), 8))
    lines_back([4], 4)

    last = pl.ds(LAST, LENGTH - LAST)
    for out, new in list(zip(home_outs, first[0])) + [(visit_out, first[1])]:
        if new:
            for h in range(2):
                out[h, :, last] = jnp.zeros((8, LENGTH - LAST), jnp.float32)

    def flat_back(tiles):
        for fold, at, width in tiles:
            vs = [down(half_back[fold], u[p, :, pl.ds(at, width)]) for p in range(pairs)]
            for h in range(2):
                for i, lanes in enumerate(lanes_of(fold, at, width)):
                    total = visit_out[h, :, lanes] if i == 4 or not first[1] else 0.0
                    other = visit[h, :, lanes]
                    for p in range(pairs):
                        part = vs[p][40 * h + 8 * i : 40 * h + 8 * (i + 1)]
                        before = home_outs[p][h, :, lanes] if i == 4 or not first[0][p] else 0.0
                        home_outs[p][h, :, lanes] = before - part * other
                        total = total - part * homes[p][h, :, lanes]
                    visit_out[h, :, lanes] = total

    loop(TAIL // WIDE // body, lambda i: flat_back(wide_tiles(i)))
    flat_back([(1, TAIL, LANES)])


HBM = pl.BlockSpec(memory_space=pl.ANY)
VMEM = pl.BlockSpec(memory_space=pltpu.VMEM)


def places():
    n, g, count = lax.axis_index("band"), lax.axis_index("grid"), lax.axis_size("band")
    core, r = lax.rem(n, 2), lax.rem(n, 4)
    swap = (n, 1 - g)
    x_to = (lax.rem(n + 2, count), 1 - g)
    x_from = (jnp.where(r == 1, n + 1, lax.rem(n + count - 2, count)), 1 - g)
    r_to = (lax.rem(n + count - 1, count), 1 - g)
    y_to, y_from = (lax.rem(n + 1 + 2 * core, count), g), (lax.rem(n + count - 3 + 2 * core, count), g)
    side = (n + 1 - 2 * core, g)
    return g, r, swap, x_to, x_from, r_to, y_to, y_from, side


def greet(senders):
    barrier = pltpu.get_barrier_semaphore()
    for use, device in senders:

        def signal():
            pl.semaphore_signal(barrier, inc=1, device_id=device, device_id_type=MESH)

        signal() if use is None else pl.when(use)(signal)


def blocked(raw, b, out):
    for i in range(4):
        out[:, LINE * i : LINE * i + PLANE] = raw[8 * i : 8 * (i + 1), b, :]
        out[:, LINE * i + PLANE : LINE * (i + 1)] = jnp.zeros((8, LINE - PLANE), jnp.float32)
    end = LAST + PLANE - FOLD
    out[:4, LAST : LAST + FOLD] = raw[32:, b, :FOLD]
    out[:4, LAST + FOLD :] = jnp.zeros((4, LENGTH - LAST - FOLD), jnp.float32)
    out[4:, LAST:end] = raw[32:, b, FOLD:]
    out[4:, end:] = jnp.zeros((4, LENGTH - end), jnp.float32)


def unblocked(part, raw, b):
    for i in range(4):
        raw[8 * i : 8 * (i + 1), b, :] = part(slice(0, 8), slice(LINE * i, LINE * i + PLANE))
    raw[32:, b, :FOLD] = part(slice(0, 4), slice(LAST, LAST + FOLD))
    raw[32:, b, FOLD:] = part(slice(4, 8), slice(LAST, LAST + PLANE - FOLD))


def sender(send, recv):
    index = iter(range(64))

    def make(src, dst, device, into=None):
        i = next(index)
        j = i if into is None else into
        copy = pltpu.make_async_remote_copy(src, dst, send.at[i], recv.at[j], device_id=device, device_id_type=MESH)
        return copy, i

    return make


def exchange_kernel(
    bands, ahead, back, half_ahead, half_back, wide_ahead, wide_back, out,
    flat, outs, lane_ahead, lane_back, factors, u, w, from_s, from_x, from_y, from_r, from_e, raw, send, recv, local,
):
    g, r, swap, x_to, x_from, r_to, y_to, y_from, side = places()
    sends_x, relays = r != 3, r == 2
    f = 1 - g
    pieces = range(len(CHUNKS))
    make = sender(send, recv)

    def cells(c):
        return pl.ds(*CHUNKS[c])

    def many(src, dst, device, into=None):
        made = [
            make(src.at[:, cells(c)], dst.at[:, cells(c)], device, None if into is None else into[c]) for c in pieces
        ]
        return [copy for copy, _ in made], [i for _, i in made]

    load = pltpu.make_async_copy(bands, raw, local.at[0])
    load.start()
    greet([(None, swap), (None, x_from), (None, y_from), (None, side)])
    load.wait()
    for b in range(2):
        blocked(raw, b, flat.at[b, g])
    pl.semaphore_wait(pltpu.get_barrier_semaphore(), 3 + jnp.where(sends_x, 1, 0) + jnp.where(relays, 1, 0))
    e1, _ = many(flat.at[g, g], flat.at[g, g], swap)
    x1, x1_at = make(flat.at[f, g], flat.at[2, g], x_to)
    y1, _ = make(flat.at[f, g], flat.at[4, g], y_to)
    e2, _ = make(flat.at[f, g], flat.at[f, g], swap)
    x2, x2_at = many(flat.at[f, f], flat.at[2, f], x_to)
    y2, _ = many(flat.at[f, f], flat.at[4, f], y_to)
    s1, _ = make(flat.at[2, f], flat.at[3, f], side)
    s2, _ = many(flat.at[2, g], flat.at[3, g], side)
    r1, _ = make(flat.at[4, g], flat.at[2, g], r_to, x1_at)
    r2, _ = many(flat.at[4, f], flat.at[2, f], r_to, x2_at)
    for copy in e1:
        copy.start()

    @pl.when(sends_x)
    def _():
        x1.start()

    y1.start()
    fill_tables(wide_ahead, wide_back, lane_ahead, lane_back, factors)
    for c in pieces:
        e1[c].wait_recv()

        @pl.when(sends_x)
        def _():
            x2[c].start()

        y2[c].start()
    e2.start()

    def pairs(homes, slot, first):
        exchange(
            [flat.at[b] for b in homes], flat.at[slot], [outs.at[b] for b in homes], outs.at[slot], first,
            (ahead, back, half_ahead, half_back), lane_ahead, lane_back, factors, u, w,
        )

    s_back = [many(outs.at[3, h], from_s.at[h], side)[0] for h in (g, f)]
    y_back = [many(outs.at[4, h], from_y.at[h], y_from)[0] for h in (f, g)]
    x_back = [many(outs.at[2, h], from_x.at[h], x_from)[0] for h in (g, f)]
    r_back = [many(outs.at[2, h], from_r.at[h], x_from)[0] for h in (g, f)]
    e1_back, _ = make(outs.at[g, f], from_e.at[g], swap)
    e2_back, _ = many(outs.at[f, f], from_e.at[f], swap)

    y1.wait_recv()

    @pl.when(relays)
    def _():
        r1.start()

    for c in pieces:
        y2[c].wait_recv()

        @pl.when(relays)
        def _():
            r2[c].start()

    pairs([f], 4, ((True,), True))
    e2.wait_recv()
    x1.wait_recv()
    s1.start()
    for c in pieces:
        x2[c].wait_recv()
        s2[c].start()
    pairs([f, g], 2, ((False, True), True))
    s1.wait_recv()
    for copy in s2:
        copy.wait_recv()
    pairs([f, g], 3, ((False, False), True))
    for copy in s_back[0] + s_back[1]:
        copy.start()
    for k, h in enumerate((g, f)):
        for c in pieces:
            s_back[k][c].wait_recv()
            outs[2, h, :, cells(c)] += from_s[h, :, cells(c)]

            @pl.when(r != 1)
            def _():
                x_back[k][c].start()

            @pl.when(r == 1)
            def _():
                r_back[k][c].start()

    pairs([g], 4, ((False,), False))
    e1_back.start()

    @pl.when(r != 2)
    def _():
        for copy in y_back[0] + y_back[1]:
            copy.start()

    for k, h in enumerate((f, g)):
        for c in pieces:

            @pl.when(relays)
            def _():
                r_back[k][c].wait_recv()
                outs[4, h, :, cells(c)] += from_r[h, :, cells(c)]
                y_back[k][c].start()

            @pl.when(sends_x)
            def _():
                x_back[k][c].wait_recv()
                outs[f, h, :, cells(c)] += from_x[h, :, cells(c)]

            y_back[k][c].wait_recv()
            outs[f, h, :, cells(c)] += from_y[h, :, cells(c)]
            if k == 0:
                e2_back[c].start()
    for copy in [e1_back] + e2_back:
        copy.wait_recv()
    for b in range(2):
        unblocked(lambda rows, lanes: outs[b, g, rows, lanes] + from_e[b, rows, lanes], raw, b)
    store = pltpu.make_async_copy(raw, out, local.at[0])
    store.start()
    store.wait()
    for copy in e1 + [y1, e2] + y2 + [s1] + s2 + s_back[0] + s_back[1] + y_back[0] + y_back[1] + [e1_back] + e2_back:
        copy.wait_send()

    @pl.when(sends_x)
    def _():
        for copy in [x1] + x2:
            copy.wait_send()

    @pl.when(relays)
    def _():
        for copy in [r1] + r2:
            copy.wait_send()

    @pl.when(r != 1)
    def _():
        for copy in x_back[0] + x_back[1]:
            copy.wait_send()

    @pl.when(r == 1)
    def _():
        for copy in r_back[0] + r_back[1]:
            copy.wait_send()


def local(bands):
    band = pltpu.VMEM((2, 8, LENGTH), jnp.float32)
    five = pltpu.VMEM((5, 2, 8, LENGTH), jnp.float32)
    table = pltpu.VMEM((8, 2, 2 * LANES, 2 * LANES), jnp.float32)
    terms = pl.pallas_call(
        exchange_kernel,
        out_shape=jax.ShapeDtypeStruct((HALF, 2, PLANE), jnp.float32),
        in_specs=[HBM] + [VMEM] * 6,
        out_specs=HBM,
        scratch_shapes=[
            five, five, table, table,
            pltpu.VMEM((ROWS, LANES), jnp.float32),
            pltpu.VMEM((2, N, LINE), jnp.float32),
            pltpu.VMEM((2, ROWS, LANES), jnp.float32),
            band, band, band, band, band,
            pltpu.VMEM((HALF, 2, PLANE), jnp.float32),
            pltpu.SemaphoreType.DMA((48,)), pltpu.SemaphoreType.DMA((48,)), pltpu.SemaphoreType.DMA((1,)),
        ],
        compiler_params=pltpu.CompilerParams(collective_id=0, has_side_effects=True, vmem_limit_bytes=63 * 1024 * 1024),
        name="exchange_terms",
    )(bands.transpose(1, 0, 2), *constants())
    return terms.transpose(1, 0, 2)


def solution(mesh):
    return jax.shard_map(
        local,
        mesh=mesh,
        in_specs=(P("band", "grid", None),),
        out_specs=P("band", "grid", None),
        check_vma=False,
    )
```

```python
import functools
import math

import jax
import jax.numpy as jnp
import numpy as np
from jax import lax
from jax.experimental import pallas as pl
from jax.experimental.pallas import tpu as pltpu
from jax.sharding import PartitionSpec as P

N = 72
HALF = 36
LANES = 128
ROWS = N * N
PLANE = N * N
MESH = pl.DeviceIdType.MESH
LINE = 41 * LANES
FOLD = 20 * LANES
LAST = 4 * LINE
LENGTH = LAST + LINE - FOLD
CHUNKS = ((0, 62 * LANES), (62 * LANES, 62 * LANES), (124 * LANES, 61 * LANES))
spacing = 0.5167


def rounded(x):
    return x.astype(jnp.bfloat16).astype(np.float32)


def constants():
    index = np.arange(N)
    freq = np.where(index <= HALF, index, index - HALF)
    phase = (freq[:, None] * index[None, :] % N) * (2.0 * math.pi / N)
    table = np.where(index[:, None] <= HALF, np.cos(phase), np.sin(phase)).astype(np.float32)

    def stacked(t):
        return np.concatenate([t, t, t - rounded(t)], axis=1)

    def blocks(m):
        wide = np.zeros((2 * N, 2 * LANES), np.float32)
        wide[:N, :N] = m
        wide[N:, LANES : LANES + N] = m
        return np.stack([rounded(wide), rounded(wide - rounded(wide))])

    halved = np.zeros((2, N, 80), np.float32)
    for fold in range(2):
        for row in range(N):
            half, r = divmod(row, HALF)
            halved[fold, :, 40 * half + r + (4 * fold if r >= 32 else 0)] = table[:, row]
    half_ahead = np.stack([stacked(m) for m in halved])
    half_back = np.stack([stacked(m.T) for m in halved])
    return stacked(table), stacked(table.T), half_ahead, half_back, blocks(table.T), blocks(table.T).transpose(0, 2, 1)


def dot(a, b):
    return jnp.dot(a, b, preferred_element_type=jnp.float32, precision=lax.Precision.DEFAULT)


def low_part(x):
    return x - x.astype(jnp.bfloat16).astype(jnp.float32)


def down(table, x):
    return dot(table, jnp.concatenate([x, low_part(x), x], axis=0))


def lanes_of(fold, at, width):
    return [pl.ds(LINE * i + at, width) for i in range(4)] + [pl.ds(LAST + at - FOLD * fold, width)]


def along(x, high, low):
    return dot(x, high) + dot(low_part(x), high) + dot(x, low)


def fill_tables(wide_ahead, wide_back, lane_ahead, lane_back, factors):
    rows = lax.broadcasted_iota(jnp.int32, (2 * N, 2 * LANES), 0)
    cols = lax.broadcasted_iota(jnp.int32, (2 * N, 2 * LANES), 1)
    for u in range(8):
        start = 2 * N * u % LANES
        move = jnp.where(cols == rows + start, 1.0, 0.0)
        for part in range(2):
            lane_ahead[u, part] = jnp.zeros((2 * LANES, 2 * LANES), jnp.float32)
            lane_ahead[u, part, start : start + 2 * N, :] = wide_ahead[part]
            lane_back[u, part] = dot(wide_back[part], move)

    def wave(i):
        f = jnp.where(i <= HALF, i, i - HALF)
        return (f * f).astype(jnp.float32), jnp.where((i == 0) | (i == HALF), 1.0, 2.0).astype(jnp.float32)

    factor = (2.0 * math.pi / (N * spacing)) ** 2
    square_b, weight_b = wave(lax.broadcasted_iota(jnp.int32, (N, LANES), 0))
    square_c, weight_c = wave(lax.broadcasted_iota(jnp.int32, (N, LANES), 1))
    inside = lax.broadcasted_iota(jnp.int32, (N, LANES), 1) < N

    def fill(i, _):
        square_a, weight_a = wave(i)
        ksq = factor * (square_a + square_b + square_c)
        keep = (ksq > 0) & inside
        coulomb = jnp.where(keep, 4.0 * math.pi / jnp.where(keep, ksq, 1.0), 0.0)
        factors[pl.ds(pl.multiple_of(i * N, 8), N), :] = coulomb * (weight_a * weight_b * weight_c) / float(N**3)
        return 0

    lax.fori_loop(0, N, fill, 0)


def exchange(homes, visit, home_outs, visit_out, first, tables, lane_ahead, lane_back, factors, u, w):
    ahead, back, half_ahead, half_back = tables
    pairs = len(homes)
    WIDE = 2 * LANES
    TAIL = PLANE // WIDE * WIDE
    tiles = [(k // 10, k * WIDE, WIDE) for k in range(TAIL // WIDE)] + [(1, TAIL, LANES)]
    strip = 18 if pairs == 2 else 12

    def flat_ahead(tiles):
        for fold, at, width in tiles:
            where = lanes_of(fold, at, width)
            for p in range(pairs):
                x = [homes[p][h, :, lanes] * visit[h, :, lanes] for h in range(2) for lanes in where]
                u[p, :, pl.ds(at, width)] = down(half_ahead[fold], jnp.concatenate(x, axis=0))

    def loop(count, work, start=0):
        def step(i, _):
            work(i)
            return 0

        lax.fori_loop(start, count, step, 0)

    flat_ahead(tiles)

    def places_of(blocks):
        return [(p, t) for t in blocks for p in range(pairs)]

    def base(t):
        return pl.multiple_of(t * 9 * LANES, LANES)

    def line(t, k):
        return pl.multiple_of((t * 8 + k) * 2 * N, 8)

    def lines_ahead(blocks, count):
        for k in range(count):
            at = 2 * N * k // LANES * LANES
            x = jnp.concatenate([u[p, :, pl.ds(base(t) + at, WIDE)] for p, t in places_of(blocks)], axis=0)
            y = along(x, lane_ahead[k, 0], lane_ahead[k, 1])
            for i, (p, t) in enumerate(places_of(blocks)):
                for half in range(2):
                    part = y[N * i : N * (i + 1), LANES * half : LANES * (half + 1)]
                    w[p, pl.ds(line(t, k) + half * N, N), :] = part

    def block_range(i):
        return [i * 4 // pairs + j for j in range(4 // pairs)]

    loop(pairs, lambda i: lines_ahead(block_range(i), 8))
    lines_ahead([4], 4)

    def at(i):
        return [(0, i), (1, i)] if pairs == 2 else [(0, 2 * i), (0, 2 * i + 1)]

    def load_w(i):
        return jnp.concatenate([w[p, pl.ds(q, N, stride=N), :] for p, q in at(i)], axis=1)

    def store_w(i, y):
        for half, (p, q) in enumerate(at(i)):
            w[p, pl.ds(q, N, stride=N), :] = y[:, LANES * half : LANES * (half + 1)]

    def ahead_b(i, x):
        y = down(ahead[...], x)
        return y * jnp.concatenate([factors[pl.ds(pl.multiple_of(q * N, 8), N), :] for _, q in at(i)], axis=1)

    def middle(i):
        now = [i * strip + k for k in range(strip)]
        before = [i * strip - strip + k for k in range(strip)]
        xs, ys = [load_w(q) for q in now], [load_w(q) for q in before]
        xs = [ahead_b(q, x) for q, x in zip(now, xs)]
        ys = [down(back[...], y) for y in ys]
        for q, x in zip(now, xs):
            store_w(q, x)
        for q, y in zip(before, ys):
            store_w(q, y)

    count = N * pairs // 2
    for q, x in [(q, ahead_b(q, load_w(q))) for q in range(strip)]:
        store_w(q, x)
    loop(count // strip, middle, 1)
    for q, y in [(q, down(back[...], load_w(q))) for q in range(count - strip, count)]:
        store_w(q, y)

    def lines_back(blocks, count):
        total = {}
        for k in range(count):
            tile = 2 * N * k // LANES
            x = jnp.concatenate(
                [
                    jnp.concatenate([w[p, pl.ds(line(t, k) + half * N, N), :] for half in range(2)], axis=1)
                    for p, t in places_of(blocks)
                ],
                axis=0,
            )
            y = along(x, lane_back[k, 0], lane_back[k, 1])
            for half in range(2):
                part = y[:, LANES * half : LANES * (half + 1)]
                total[tile + half] = total[tile + half] + part if tile + half in total else part
        for tile, value in total.items():
            for i, (p, t) in enumerate(places_of(blocks)):
                u[p, :, pl.ds(base(t) + tile * LANES, LANES)] = value[N * i : N * (i + 1)]

    loop(pairs, lambda i: lines_back(block_range(i), 8))
    lines_back([4], 4)

    last = pl.ds(LAST, LENGTH - LAST)
    for out, new in list(zip(home_outs, first[0])) + [(visit_out, first[1])]:
        if new:
            for h in range(2):
                out[h, :, last] = jnp.zeros((8, LENGTH - LAST), jnp.float32)

    def flat_back(tiles):
        for fold, at, width in tiles:
            vs = [down(half_back[fold], u[p, :, pl.ds(at, width)]) for p in range(pairs)]
            for h in range(2):
                for i, lanes in enumerate(lanes_of(fold, at, width)):
                    total = visit_out[h, :, lanes] if i == 4 or not first[1] else 0.0
                    other = visit[h, :, lanes]
                    for p in range(pairs):
                        part = vs[p][40 * h + 8 * i : 40 * h + 8 * (i + 1)]
                        before = home_outs[p][h, :, lanes] if i == 4 or not first[0][p] else 0.0
                        home_outs[p][h, :, lanes] = before - part * other
                        total = total - part * homes[p][h, :, lanes]
                    visit_out[h, :, lanes] = total

    flat_back(tiles)


HBM = pl.BlockSpec(memory_space=pl.ANY)
VMEM = pl.BlockSpec(memory_space=pltpu.VMEM)


def places():
    n, g, count = lax.axis_index("band"), lax.axis_index("grid"), lax.axis_size("band")
    core, r = lax.rem(n, 2), lax.rem(n, 4)
    swap = (n, 1 - g)
    x_to = (lax.rem(n + 2, count), 1 - g)
    x_from = (jnp.where(r == 1, n + 1, lax.rem(n + count - 2, count)), 1 - g)
    r_to = (lax.rem(n + count - 1, count), 1 - g)
    y_to, y_from = (lax.rem(n + 1 + 2 * core, count), g), (lax.rem(n + count - 3 + 2 * core, count), g)
    side = (n + 1 - 2 * core, g)
    return g, r, swap, x_to, x_from, r_to, y_to, y_from, side


def greet(senders):
    barrier = pltpu.get_barrier_semaphore()
    for use, device in senders:

        def signal():
            pl.semaphore_signal(barrier, inc=1, device_id=device, device_id_type=MESH)

        signal() if use is None else pl.when(use)(signal)


def blocked(raw, b, out):
    for i in range(4):
        out[:, LINE * i : LINE * i + PLANE] = raw[8 * i : 8 * (i + 1), b, :]
        out[:, LINE * i + PLANE : LINE * (i + 1)] = jnp.zeros((8, LINE - PLANE), jnp.float32)
    end = LAST + PLANE - FOLD
    out[:4, LAST : LAST + FOLD] = raw[32:, b, :FOLD]
    out[:4, LAST + FOLD :] = jnp.zeros((4, LENGTH - LAST - FOLD), jnp.float32)
    out[4:, LAST:end] = raw[32:, b, FOLD:]
    out[4:, end:] = jnp.zeros((4, LENGTH - end), jnp.float32)


def unblocked(part, raw, b):
    for i in range(4):
        raw[8 * i : 8 * (i + 1), b, :] = part(slice(0, 8), slice(LINE * i, LINE * i + PLANE))
    raw[32:, b, :FOLD] = part(slice(0, 4), slice(LAST, LAST + FOLD))
    raw[32:, b, FOLD:] = part(slice(4, 8), slice(LAST, LAST + PLANE - FOLD))


def sender(send, recv):
    index = iter(range(64))

    def make(src, dst, device, into=None):
        i = next(index)
        j = i if into is None else into
        copy = pltpu.make_async_remote_copy(src, dst, send.at[i], recv.at[j], device_id=device, device_id_type=MESH)
        return copy, i

    return make


def exchange_kernel(
    bands, ahead, back, half_ahead, half_back, wide_ahead, wide_back, out,
    flat, outs, lane_ahead, lane_back, factors, u, w, from_s, from_x, from_y, from_r, from_e, raw, send, recv, local,
):
    g, r, swap, x_to, x_from, r_to, y_to, y_from, side = places()
    sends_x, relays = r != 3, r == 2
    f = 1 - g
    pieces = range(len(CHUNKS))
    make = sender(send, recv)

    def cells(c):
        return pl.ds(*CHUNKS[c])

    def many(src, dst, device, into=None):
        made = [
            make(src.at[:, cells(c)], dst.at[:, cells(c)], device, None if into is None else into[c]) for c in pieces
        ]
        return [copy for copy, _ in made], [i for _, i in made]

    load = pltpu.make_async_copy(bands, raw, local.at[0])
    load.start()
    greet([(None, swap), (None, x_from), (None, y_from), (None, side)])
    load.wait()
    for b in range(2):
        blocked(raw, b, flat.at[b, g])
    pl.semaphore_wait(pltpu.get_barrier_semaphore(), 3 + jnp.where(sends_x, 1, 0) + jnp.where(relays, 1, 0))
    e1, _ = many(flat.at[g, g], flat.at[g, g], swap)
    x1, x1_at = make(flat.at[f, g], flat.at[2, g], x_to)
    y1, _ = make(flat.at[f, g], flat.at[4, g], y_to)
    e2, _ = make(flat.at[f, g], flat.at[f, g], swap)
    x2, x2_at = many(flat.at[f, f], flat.at[2, f], x_to)
    y2, _ = many(flat.at[f, f], flat.at[4, f], y_to)
    s1, _ = make(flat.at[2, f], flat.at[3, f], side)
    s2, _ = many(flat.at[2, g], flat.at[3, g], side)
    r1, _ = make(flat.at[4, g], flat.at[2, g], r_to, x1_at)
    r2, _ = many(flat.at[4, f], flat.at[2, f], r_to, x2_at)
    for copy in e1:
        copy.start()

    @pl.when(sends_x)
    def _():
        x1.start()

    y1.start()
    fill_tables(wide_ahead, wide_back, lane_ahead, lane_back, factors)
    for c in pieces:
        e1[c].wait_recv()

        @pl.when(sends_x)
        def _():
            x2[c].start()

        y2[c].start()
    e2.start()

    def pairs(homes, slot, first):
        exchange(
            [flat.at[b] for b in homes], flat.at[slot], [outs.at[b] for b in homes], outs.at[slot], first,
            (ahead, back, half_ahead, half_back), lane_ahead, lane_back, factors, u, w,
        )

    s_back = [many(outs.at[3, h], from_s.at[h], side)[0] for h in (g, f)]
    y_back = [many(outs.at[4, h], from_y.at[h], y_from)[0] for h in (f, g)]
    x_back = [many(outs.at[2, h], from_x.at[h], x_from)[0] for h in (g, f)]
    r_back = [many(outs.at[2, h], from_r.at[h], x_from)[0] for h in (g, f)]
    e1_back, _ = make(outs.at[g, f], from_e.at[g], swap)
    e2_back, _ = many(outs.at[f, f], from_e.at[f], swap)

    y1.wait_recv()

    @pl.when(relays)
    def _():
        r1.start()

    for c in pieces:
        y2[c].wait_recv()

        @pl.when(relays)
        def _():
            r2[c].start()

    outs[4] = jnp.zeros((2, 8, LENGTH), jnp.float32)

    def with_y(i, _):
        @pl.when(i == 1)
        def _():
            e2.wait_recv()

        pairs([lax.rem(f + i, 2)], 4, ((True,), False))
        return 0

    lax.fori_loop(0, 2, with_y, 0)

    @pl.when(r != 2)
    def _():
        for copy in y_back[0] + y_back[1]:
            copy.start()

    x1.wait_recv()
    s1.start()
    for c in pieces:
        x2[c].wait_recv()
        s2[c].start()

    def with_x_and_s(i, _):
        @pl.when(i == 1)
        def _():
            for copy in [s1] + s2:
                copy.wait_recv()

        pairs([0, 1], 2 + i, ((False, False), True))
        return 0

    lax.fori_loop(0, 2, with_x_and_s, 0)
    for copy in s_back[0] + s_back[1]:
        copy.start()
    e1_back.start()
    for k, h in enumerate((g, f)):
        for c in pieces:
            s_back[k][c].wait_recv()
            outs[2, h, :, cells(c)] += from_s[h, :, cells(c)]

            @pl.when(r != 1)
            def _():
                x_back[k][c].start()

            @pl.when(r == 1)
            def _():
                r_back[k][c].start()

    for k, h in enumerate((f, g)):
        for c in pieces:

            @pl.when(relays)
            def _():
                r_back[k][c].wait_recv()
                outs[4, h, :, cells(c)] += from_r[h, :, cells(c)]
                y_back[k][c].start()

            @pl.when(sends_x)
            def _():
                x_back[k][c].wait_recv()
                outs[f, h, :, cells(c)] += from_x[h, :, cells(c)]

            y_back[k][c].wait_recv()
            outs[f, h, :, cells(c)] += from_y[h, :, cells(c)]
            if k == 0:
                e2_back[c].start()
    for copy in [e1_back] + e2_back:
        copy.wait_recv()
    for b in range(2):
        unblocked(lambda rows, lanes: outs[b, g, rows, lanes] + from_e[b, rows, lanes], raw, b)
    store = pltpu.make_async_copy(raw, out, local.at[0])
    store.start()
    store.wait()
    for copy in e1 + [y1, e2] + y2 + [s1] + s2 + s_back[0] + s_back[1] + y_back[0] + y_back[1] + [e1_back] + e2_back:
        copy.wait_send()

    @pl.when(sends_x)
    def _():
        for copy in [x1] + x2:
            copy.wait_send()

    @pl.when(relays)
    def _():
        for copy in [r1] + r2:
            copy.wait_send()

    @pl.when(r != 1)
    def _():
        for copy in x_back[0] + x_back[1]:
            copy.wait_send()

    @pl.when(r == 1)
    def _():
        for copy in r_back[0] + r_back[1]:
            copy.wait_send()


def local(bands):
    band = pltpu.VMEM((2, 8, LENGTH), jnp.float32)
    five = pltpu.VMEM((5, 2, 8, LENGTH), jnp.float32)
    table = pltpu.VMEM((8, 2, 2 * LANES, 2 * LANES), jnp.float32)
    terms = pl.pallas_call(
        exchange_kernel,
        out_shape=jax.ShapeDtypeStruct((HALF, 2, PLANE), jnp.float32),
        in_specs=[HBM] + [VMEM] * 6,
        out_specs=HBM,
        scratch_shapes=[
            five, five, table, table,
            pltpu.VMEM((ROWS, LANES), jnp.float32),
            pltpu.VMEM((2, N, LINE), jnp.float32),
            pltpu.VMEM((2, ROWS, LANES), jnp.float32),
            band, band, band, band, band,
            pltpu.VMEM((HALF, 2, PLANE), jnp.float32),
            pltpu.SemaphoreType.DMA((48,)), pltpu.SemaphoreType.DMA((48,)), pltpu.SemaphoreType.DMA((1,)),
        ],
        compiler_params=pltpu.CompilerParams(collective_id=0, has_side_effects=True, vmem_limit_bytes=63 * 1024 * 1024),
        name="exchange_terms",
    )(bands.transpose(1, 0, 2), *constants())
    return terms.transpose(1, 0, 2)


def solution(mesh):
    return jax.shard_map(
        local,
        mesh=mesh,
        in_specs=(P("band", "grid", None),),
        out_specs=P("band", "grid", None),
        check_vma=False,
    )
```

```python
import functools
import math

import jax
import jax.numpy as jnp
import numpy as np
from jax import lax
from jax.experimental import pallas as pl
from jax.experimental.pallas import tpu as pltpu
from jax.sharding import PartitionSpec as P

N = 72
HALF = 36
LANES = 128
ROWS = N * N
PLANE = N * N
MESH = pl.DeviceIdType.MESH
LINE = 41 * LANES
FOLD = 20 * LANES
LAST = 4 * LINE
LENGTH = LAST + LINE - FOLD
CHUNKS = ((0, 46 * LANES), (46 * LANES, 46 * LANES), (92 * LANES, 46 * LANES), (138 * LANES, 47 * LANES))
spacing = 0.5167


def rounded(x):
    return x.astype(jnp.bfloat16).astype(np.float32)


def constants():
    index = np.arange(N)
    freq = np.where(index <= HALF, index, index - HALF)
    phase = (freq[:, None] * index[None, :] % N) * (2.0 * math.pi / N)
    table = np.where(index[:, None] <= HALF, np.cos(phase), np.sin(phase)).astype(np.float32)

    def stacked(t):
        return np.concatenate([t, t, t - rounded(t)], axis=1)

    def blocks(m):
        wide = np.zeros((2 * N, 2 * LANES), np.float32)
        wide[:N, :N] = m
        wide[N:, LANES : LANES + N] = m
        return np.stack([rounded(wide), rounded(wide - rounded(wide))])

    halved = np.zeros((2, N, 80), np.float32)
    for fold in range(2):
        for row in range(N):
            half, r = divmod(row, HALF)
            halved[fold, :, 40 * half + r + (4 * fold if r >= 32 else 0)] = table[:, row]
    half_ahead = np.stack([stacked(m) for m in halved])
    half_back = np.stack([stacked(m.T) for m in halved])
    return stacked(table), stacked(table.T), half_ahead, half_back, blocks(table.T), blocks(table.T).transpose(0, 2, 1)


def dot(a, b):
    return jnp.dot(a, b, preferred_element_type=jnp.float32, precision=lax.Precision.DEFAULT)


def low_part(x):
    return x - x.astype(jnp.bfloat16).astype(jnp.float32)


def down(table, x):
    return dot(table, jnp.concatenate([x, low_part(x), x], axis=0))


def lanes_of(fold, at, width):
    return [pl.ds(LINE * i + at, width) for i in range(4)] + [pl.ds(LAST + at - FOLD * fold, width)]


def along(x, high, low):
    return dot(x, high) + dot(low_part(x), high) + dot(x, low)


def fill_tables(wide_ahead, wide_back, lane_ahead, lane_back, factors):
    rows = lax.broadcasted_iota(jnp.int32, (2 * N, 2 * LANES), 0)
    cols = lax.broadcasted_iota(jnp.int32, (2 * N, 2 * LANES), 1)
    for u in range(8):
        start = 2 * N * u % LANES
        move = jnp.where(cols == rows + start, 1.0, 0.0)
        for part in range(2):
            lane_ahead[u, part] = jnp.zeros((2 * LANES, 2 * LANES), jnp.float32)
            lane_ahead[u, part, start : start + 2 * N, :] = wide_ahead[part]
            lane_back[u, part] = dot(wide_back[part], move)

    def wave(i):
        f = jnp.where(i <= HALF, i, i - HALF)
        return (f * f).astype(jnp.float32), jnp.where((i == 0) | (i == HALF), 1.0, 2.0).astype(jnp.float32)

    factor = (2.0 * math.pi / (N * spacing)) ** 2
    square_b, weight_b = wave(lax.broadcasted_iota(jnp.int32, (N, LANES), 0))
    square_c, weight_c = wave(lax.broadcasted_iota(jnp.int32, (N, LANES), 1))
    inside = lax.broadcasted_iota(jnp.int32, (N, LANES), 1) < N

    def fill(i, _):
        square_a, weight_a = wave(i)
        ksq = factor * (square_a + square_b + square_c)
        keep = (ksq > 0) & inside
        coulomb = jnp.where(keep, 4.0 * math.pi / jnp.where(keep, ksq, 1.0), 0.0)
        factors[pl.ds(pl.multiple_of(i * N, 8), N), :] = coulomb * (weight_a * weight_b * weight_c) / float(N**3)
        return 0

    lax.fori_loop(0, N, fill, 0)


def exchange(homes, visit, home_outs, visit_out, first, tables, lane_ahead, lane_back, factors, u, w):
    ahead, back, half_ahead, half_back = tables
    pairs = len(homes)
    WIDE = 2 * LANES
    TAIL = PLANE // WIDE * WIDE
    tiles = [(k // 10, k * WIDE, WIDE) for k in range(TAIL // WIDE)] + [(1, TAIL, LANES)]
    strip = 18 if pairs == 2 else 12

    def flat_ahead(tiles):
        for fold, at, width in tiles:
            where = lanes_of(fold, at, width)
            for p in range(pairs):
                x = [homes[p][h, :, lanes] * visit[h, :, lanes] for h in range(2) for lanes in where]
                u[p, :, pl.ds(at, width)] = down(half_ahead[fold], jnp.concatenate(x, axis=0))

    def loop(count, work, start=0):
        def step(i, _):
            work(i)
            return 0

        lax.fori_loop(start, count, step, 0)

    flat_ahead(tiles)

    def places_of(blocks):
        return [(p, t) for t in blocks for p in range(pairs)]

    def base(t):
        return pl.multiple_of(t * 9 * LANES, LANES)

    def line(t, k):
        return pl.multiple_of((t * 8 + k) * 2 * N, 8)

    def lines_ahead(blocks, count):
        for k in range(count):
            at = 2 * N * k // LANES * LANES
            x = jnp.concatenate([u[p, :, pl.ds(base(t) + at, WIDE)] for p, t in places_of(blocks)], axis=0)
            y = along(x, lane_ahead[k, 0], lane_ahead[k, 1])
            for i, (p, t) in enumerate(places_of(blocks)):
                for half in range(2):
                    part = y[N * i : N * (i + 1), LANES * half : LANES * (half + 1)]
                    w[p, pl.ds(line(t, k) + half * N, N), :] = part

    def block_range(i):
        return list(range(4))

    loop(1, lambda i: lines_ahead(block_range(i), 8))
    lines_ahead([4], 4)

    def at(i):
        return [(0, i), (1, i)] if pairs == 2 else [(0, 2 * i), (0, 2 * i + 1)]

    def load_w(i):
        return jnp.concatenate([w[p, pl.ds(q, N, stride=N), :] for p, q in at(i)], axis=1)

    def store_w(i, y):
        for half, (p, q) in enumerate(at(i)):
            w[p, pl.ds(q, N, stride=N), :] = y[:, LANES * half : LANES * (half + 1)]

    def ahead_b(i, x):
        y = down(ahead[...], x)
        return y * jnp.concatenate([factors[pl.ds(pl.multiple_of(q * N, 8), N), :] for _, q in at(i)], axis=1)

    def middle(i):
        now = [i * strip + k for k in range(strip)]
        before = [i * strip - strip + k for k in range(strip)]
        xs, ys = [load_w(q) for q in now], [load_w(q) for q in before]
        xs = [ahead_b(q, x) for q, x in zip(now, xs)]
        ys = [down(back[...], y) for y in ys]
        for q, x in zip(now, xs):
            store_w(q, x)
        for q, y in zip(before, ys):
            store_w(q, y)

    count = N * pairs // 2
    for q, x in [(q, ahead_b(q, load_w(q))) for q in range(strip)]:
        store_w(q, x)
    loop(count // strip, middle, 1)
    for q, y in [(q, down(back[...], load_w(q))) for q in range(count - strip, count)]:
        store_w(q, y)

    def lines_back(blocks, count):
        total = {}
        for k in range(count):
            tile = 2 * N * k // LANES
            x = jnp.concatenate(
                [
                    jnp.concatenate([w[p, pl.ds(line(t, k) + half * N, N), :] for half in range(2)], axis=1)
                    for p, t in places_of(blocks)
                ],
                axis=0,
            )
            y = along(x, lane_back[k, 0], lane_back[k, 1])
            for half in range(2):
                part = y[:, LANES * half : LANES * (half + 1)]
                total[tile + half] = total[tile + half] + part if tile + half in total else part
        for tile, value in total.items():
            for i, (p, t) in enumerate(places_of(blocks)):
                u[p, :, pl.ds(base(t) + tile * LANES, LANES)] = value[N * i : N * (i + 1)]

    loop(1, lambda i: lines_back(block_range(i), 8))
    lines_back([4], 4)

    last = pl.ds(LAST, LENGTH - LAST)
    for out, new in list(zip(home_outs, first[0])) + [(visit_out, first[1])]:
        if new:
            for h in range(2):
                out[h, :, last] = jnp.zeros((8, LENGTH - LAST), jnp.float32)

    def flat_back(tiles):
        for fold, at, width in tiles:
            vs = [down(half_back[fold], u[p, :, pl.ds(at, width)]) for p in range(pairs)]
            for h in range(2):
                for i, lanes in enumerate(lanes_of(fold, at, width)):
                    total = visit_out[h, :, lanes] if i == 4 or not first[1] else 0.0
                    other = visit[h, :, lanes]
                    for p in range(pairs):
                        part = vs[p][40 * h + 8 * i : 40 * h + 8 * (i + 1)]
                        before = home_outs[p][h, :, lanes] if i == 4 or not first[0][p] else 0.0
                        home_outs[p][h, :, lanes] = before - part * other
                        total = total - part * homes[p][h, :, lanes]
                    visit_out[h, :, lanes] = total

    flat_back(tiles)


HBM = pl.BlockSpec(memory_space=pl.ANY)
VMEM = pl.BlockSpec(memory_space=pltpu.VMEM)


def places():
    n, g, count = lax.axis_index("band"), lax.axis_index("grid"), lax.axis_size("band")
    core, r = lax.rem(n, 2), lax.rem(n, 4)
    swap = (n, 1 - g)
    x_to = (lax.rem(n + 2, count), 1 - g)
    x_from = (jnp.where(r == 1, n + 1, lax.rem(n + count - 2, count)), 1 - g)
    r_to = (lax.rem(n + count - 1, count), 1 - g)
    y_to, y_from = (lax.rem(n + 1 + 2 * core, count), g), (lax.rem(n + count - 3 + 2 * core, count), g)
    side = (n + 1 - 2 * core, g)
    return g, r, swap, x_to, x_from, r_to, y_to, y_from, side


def greet(senders):
    barrier = pltpu.get_barrier_semaphore()
    for use, device in senders:

        def signal():
            pl.semaphore_signal(barrier, inc=1, device_id=device, device_id_type=MESH)

        signal() if use is None else pl.when(use)(signal)


def blocked(raw, b, out):
    for i in range(4):
        out[:, LINE * i : LINE * i + PLANE] = raw[8 * i : 8 * (i + 1), b, :]
        out[:, LINE * i + PLANE : LINE * (i + 1)] = jnp.zeros((8, LINE - PLANE), jnp.float32)
    end = LAST + PLANE - FOLD
    out[:4, LAST : LAST + FOLD] = raw[32:, b, :FOLD]
    out[:4, LAST + FOLD :] = jnp.zeros((4, LENGTH - LAST - FOLD), jnp.float32)
    out[4:, LAST:end] = raw[32:, b, FOLD:]
    out[4:, end:] = jnp.zeros((4, LENGTH - end), jnp.float32)


def unblocked(part, raw, b):
    for i in range(4):
        raw[8 * i : 8 * (i + 1), b, :] = part(slice(0, 8), slice(LINE * i, LINE * i + PLANE))
    raw[32:, b, :FOLD] = part(slice(0, 4), slice(LAST, LAST + FOLD))
    raw[32:, b, FOLD:] = part(slice(4, 8), slice(LAST, LAST + PLANE - FOLD))


def sender(send, recv):
    index = iter(range(64))

    def make(src, dst, device, into=None):
        i = next(index)
        j = i if into is None else into
        copy = pltpu.make_async_remote_copy(src, dst, send.at[i], recv.at[j], device_id=device, device_id_type=MESH)
        return copy, i

    return make


def exchange_kernel(
    bands, ahead, back, half_ahead, half_back, wide_ahead, wide_back, out,
    flat, outs, lane_ahead, lane_back, factors, u, w, from_s, from_x, from_y, from_r, from_e, raw, send, recv, local,
):
    g, r, swap, x_to, x_from, r_to, y_to, y_from, side = places()
    sends_x, relays = r != 3, r == 2
    f = 1 - g
    pieces = range(len(CHUNKS))
    make = sender(send, recv)

    def cells(c):
        return pl.ds(*CHUNKS[c])

    def many(src, dst, device, into=None):
        made = [
            make(src.at[:, cells(c)], dst.at[:, cells(c)], device, None if into is None else into[c]) for c in pieces
        ]
        return [copy for copy, _ in made], [i for _, i in made]

    load = pltpu.make_async_copy(bands, raw, local.at[0])
    load.start()
    greet([(None, swap), (None, x_from), (None, y_from), (None, side)])
    load.wait()
    for b in range(2):
        blocked(raw, b, flat.at[b, g])
    pl.semaphore_wait(pltpu.get_barrier_semaphore(), 3 + jnp.where(sends_x, 1, 0) + jnp.where(relays, 1, 0))
    e1, _ = many(flat.at[g, g], flat.at[g, g], swap)
    x1, x1_at = make(flat.at[f, g], flat.at[2, g], x_to)
    y1, _ = make(flat.at[f, g], flat.at[4, g], y_to)
    e2, _ = make(flat.at[f, g], flat.at[f, g], swap)
    x2, x2_at = many(flat.at[f, f], flat.at[2, f], x_to)
    y2, _ = many(flat.at[f, f], flat.at[4, f], y_to)
    s1, _ = make(flat.at[2, f], flat.at[3, f], side)
    s2, _ = many(flat.at[2, g], flat.at[3, g], side)
    r1, _ = make(flat.at[4, g], flat.at[2, g], r_to, x1_at)
    r2, _ = many(flat.at[4, f], flat.at[2, f], r_to, x2_at)
    for copy in e1:
        copy.start()

    @pl.when(sends_x)
    def _():
        x1.start()

    y1.start()
    fill_tables(wide_ahead, wide_back, lane_ahead, lane_back, factors)
    for c in pieces:
        e1[c].wait_recv()

        @pl.when(sends_x)
        def _():
            x2[c].start()

        y2[c].start()
    e2.start()

    def pairs(homes, slot, first):
        exchange(
            [flat.at[b] for b in homes], flat.at[slot], [outs.at[b] for b in homes], outs.at[slot], first,
            (ahead, back, half_ahead, half_back), lane_ahead, lane_back, factors, u, w,
        )

    s_back = [many(outs.at[3, h], from_s.at[h], side)[0] for h in (g, f)]
    y_back = [many(outs.at[4, h], from_y.at[h], y_from)[0] for h in (f, g)]
    x_back = [many(outs.at[2, h], from_x.at[h], x_from)[0] for h in (g, f)]
    r_back = [many(outs.at[2, h], from_r.at[h], x_from)[0] for h in (g, f)]
    e1_back, _ = make(outs.at[g, f], from_e.at[g], swap)
    e2_back, _ = many(outs.at[f, f], from_e.at[f], swap)

    y1.wait_recv()

    @pl.when(relays)
    def _():
        r1.start()

    for c in pieces:
        y2[c].wait_recv()

        @pl.when(relays)
        def _():
            r2[c].start()

    outs[4] = jnp.zeros((2, 8, LENGTH), jnp.float32)

    def with_y(i, _):
        @pl.when(i == 1)
        def _():
            e2.wait_recv()

        pairs([lax.rem(f + i, 2)], 4, ((True,), False))
        return 0

    lax.fori_loop(0, 2, with_y, 0)

    @pl.when(r != 2)
    def _():
        for copy in y_back[0] + y_back[1]:
            copy.start()

    x1.wait_recv()
    s1.start()
    for c in pieces:
        x2[c].wait_recv()
        s2[c].start()

    def with_x_and_s(i, _):
        @pl.when(i == 1)
        def _():
            for copy in [s1] + s2:
                copy.wait_recv()

        pairs([0, 1], 2 + i, ((False, False), True))
        return 0

    lax.fori_loop(0, 2, with_x_and_s, 0)
    for copy in s_back[0] + s_back[1]:
        copy.start()
    e1_back.start()
    for k, h in enumerate((g, f)):
        for c in pieces:
            s_back[k][c].wait_recv()
            outs[2, h, :, cells(c)] += from_s[h, :, cells(c)]

            @pl.when(r != 1)
            def _():
                x_back[k][c].start()

            @pl.when(r == 1)
            def _():
                r_back[k][c].start()

    for k, h in enumerate((f, g)):
        for c in pieces:

            @pl.when(relays)
            def _():
                r_back[k][c].wait_recv()
                outs[4, h, :, cells(c)] += from_r[h, :, cells(c)]
                y_back[k][c].start()

            @pl.when(sends_x)
            def _():
                x_back[k][c].wait_recv()
                outs[f, h, :, cells(c)] += from_x[h, :, cells(c)]

            y_back[k][c].wait_recv()
            outs[f, h, :, cells(c)] += from_y[h, :, cells(c)]
            if k == 0:
                e2_back[c].start()
    for copy in [e1_back] + e2_back:
        copy.wait_recv()
    for b in range(2):
        unblocked(lambda rows, lanes: outs[b, g, rows, lanes] + from_e[b, rows, lanes], raw, b)
    store = pltpu.make_async_copy(raw, out, local.at[0])
    store.start()
    store.wait()
    for copy in e1 + [y1, e2] + y2 + [s1] + s2 + s_back[0] + s_back[1] + y_back[0] + y_back[1] + [e1_back] + e2_back:
        copy.wait_send()

    @pl.when(sends_x)
    def _():
        for copy in [x1] + x2:
            copy.wait_send()

    @pl.when(relays)
    def _():
        for copy in [r1] + r2:
            copy.wait_send()

    @pl.when(r != 1)
    def _():
        for copy in x_back[0] + x_back[1]:
            copy.wait_send()

    @pl.when(r == 1)
    def _():
        for copy in r_back[0] + r_back[1]:
            copy.wait_send()


def local(bands):
    band = pltpu.VMEM((2, 8, LENGTH), jnp.float32)
    five = pltpu.VMEM((5, 2, 8, LENGTH), jnp.float32)
    table = pltpu.VMEM((8, 2, 2 * LANES, 2 * LANES), jnp.float32)
    terms = pl.pallas_call(
        exchange_kernel,
        out_shape=jax.ShapeDtypeStruct((HALF, 2, PLANE), jnp.float32),
        in_specs=[HBM] + [VMEM] * 6,
        out_specs=HBM,
        scratch_shapes=[
            five, five, table, table,
            pltpu.VMEM((ROWS, LANES), jnp.float32),
            pltpu.VMEM((2, N, LINE), jnp.float32),
            pltpu.VMEM((2, ROWS, LANES), jnp.float32),
            band, band, band, band, band,
            pltpu.VMEM((HALF, 2, PLANE), jnp.float32),
            pltpu.SemaphoreType.DMA((64,)), pltpu.SemaphoreType.DMA((64,)), pltpu.SemaphoreType.DMA((1,)),
        ],
        compiler_params=pltpu.CompilerParams(collective_id=0, has_side_effects=True, vmem_limit_bytes=63 * 1024 * 1024),
        name="exchange_terms",
    )(bands.transpose(1, 0, 2), *constants())
    return terms.transpose(1, 0, 2)


def solution(mesh):
    return jax.shard_map(
        local,
        mesh=mesh,
        in_specs=(P("band", "grid", None),),
        out_specs=P("band", "grid", None),
        check_vma=False,
    )
```

```python
import functools
import math

import jax
import jax.numpy as jnp
import numpy as np
from jax import lax
from jax.experimental import pallas as pl
from jax.experimental.pallas import tpu as pltpu
from jax.sharding import PartitionSpec as P

N = 72
HALF = 36
LANES = 128
ROWS = N * N
PLANE = N * N
MESH = pl.DeviceIdType.MESH
LINE = 41 * LANES
FOLD = 20 * LANES
LAST = 4 * LINE
LENGTH = LAST + LINE - FOLD
CHUNKS = ((0, 46 * LANES), (46 * LANES, 46 * LANES), (92 * LANES, 46 * LANES), (138 * LANES, 47 * LANES))
spacing = 0.5167


def rounded(x):
    return x.astype(jnp.bfloat16).astype(np.float32)


def constants():
    index = np.arange(N)
    freq = np.where(index <= HALF, index, index - HALF)
    phase = (freq[:, None] * index[None, :] % N) * (2.0 * math.pi / N)
    table = np.where(index[:, None] <= HALF, np.cos(phase), np.sin(phase)).astype(np.float32)

    def stacked(t):
        return np.concatenate([t, t, t - rounded(t)], axis=1)

    def blocks(m):
        wide = np.zeros((2 * N, 2 * LANES), np.float32)
        wide[:N, :N] = m
        wide[N:, LANES : LANES + N] = m
        return np.stack([rounded(wide), rounded(wide - rounded(wide))])

    halved = np.zeros((2, N, 80), np.float32)
    for fold in range(2):
        for row in range(N):
            half, r = divmod(row, HALF)
            halved[fold, :, 40 * half + r + (4 * fold if r >= 32 else 0)] = table[:, row]
    half_ahead = np.stack([stacked(m) for m in halved])
    half_back = np.stack([stacked(m.T) for m in halved])
    return stacked(table), stacked(table.T), half_ahead, half_back, blocks(table.T), blocks(table.T).transpose(0, 2, 1)


def dot(a, b):
    return jnp.dot(a, b, preferred_element_type=jnp.float32, precision=lax.Precision.DEFAULT)


def low_part(x):
    return x - x.astype(jnp.bfloat16).astype(jnp.float32)


def down(table, x):
    return dot(table, jnp.concatenate([x, low_part(x), x], axis=0))


def lanes_of(fold, at, width):
    return [pl.ds(LINE * i + at, width) for i in range(4)] + [pl.ds(LAST + at - FOLD * fold, width)]


def along(x, high, low):
    return dot(x, high) + dot(low_part(x), high) + dot(x, low)


def fill_tables(wide_ahead, wide_back, lane_ahead, lane_back, factors):
    rows = lax.broadcasted_iota(jnp.int32, (2 * N, 2 * LANES), 0)
    cols = lax.broadcasted_iota(jnp.int32, (2 * N, 2 * LANES), 1)
    for u in range(8):
        start = 2 * N * u % LANES
        move = jnp.where(cols == rows + start, 1.0, 0.0)
        for part in range(2):
            lane_ahead[u, part] = jnp.zeros((2 * LANES, 2 * LANES), jnp.float32)
            lane_ahead[u, part, start : start + 2 * N, :] = wide_ahead[part]
            lane_back[u, part] = dot(wide_back[part], move)

    def wave(i):
        f = jnp.where(i <= HALF, i, i - HALF)
        return (f * f).astype(jnp.float32), jnp.where((i == 0) | (i == HALF), 1.0, 2.0).astype(jnp.float32)

    factor = (2.0 * math.pi / (N * spacing)) ** 2
    square_b, weight_b = wave(lax.broadcasted_iota(jnp.int32, (N, LANES), 0))
    square_c, weight_c = wave(lax.broadcasted_iota(jnp.int32, (N, LANES), 1))
    inside = lax.broadcasted_iota(jnp.int32, (N, LANES), 1) < N

    def fill(i, _):
        square_a, weight_a = wave(i)
        ksq = factor * (square_a + square_b + square_c)
        keep = (ksq > 0) & inside
        coulomb = jnp.where(keep, 4.0 * math.pi / jnp.where(keep, ksq, 1.0), 0.0)
        factors[pl.ds(pl.multiple_of(i * N, 8), N), :] = coulomb * (weight_a * weight_b * weight_c) / float(N**3)
        return 0

    lax.fori_loop(0, N, fill, 0)


def exchange(homes, visit, home_outs, visit_out, first, tables, lane_ahead, lane_back, factors, u, w):
    ahead, back, half_ahead, half_back = tables
    pairs = len(homes)
    WIDE = 2 * LANES
    TAIL = PLANE // WIDE * WIDE
    tiles = [(k // 10, k * WIDE, WIDE) for k in range(TAIL // WIDE)] + [(1, TAIL, LANES)]
    strip = 18 if pairs == 2 else 12

    def flat_ahead(tiles):
        for fold, at, width in tiles:
            where = lanes_of(fold, at, width)
            for p in range(pairs):
                x = [homes[p][h, :, lanes] * visit[h, :, lanes] for h in range(2) for lanes in where]
                u[p, :, pl.ds(at, width)] = down(half_ahead[fold], jnp.concatenate(x, axis=0))

    def loop(count, work, start=0):
        def step(i, _):
            work(i)
            return 0

        lax.fori_loop(start, count, step, 0)

    flat_ahead(tiles)

    def places_of(blocks):
        return [(p, t) for t in blocks for p in range(pairs)]

    def base(t):
        return t * 9 * LANES

    def line(t, k):
        return (t * 8 + k) * 2 * N

    def blocks_with(k):
        return range(5) if k < 4 else range(4)

    for k in range(8):
        at = 2 * N * k // LANES * LANES
        where = places_of(blocks_with(k))
        x = jnp.concatenate([u[p, :, pl.ds(base(t) + at, WIDE)] for p, t in where], axis=0)
        y = along(x, lane_ahead[k, 0], lane_ahead[k, 1])
        for i, (p, t) in enumerate(where):
            for half in range(2):
                part = y[N * i : N * (i + 1), LANES * half : LANES * (half + 1)]
                w[p, pl.ds(line(t, k) + half * N, N), :] = part

    def at(i):
        return [(0, i), (1, i)] if pairs == 2 else [(0, 2 * i), (0, 2 * i + 1)]

    def load_w(i):
        return jnp.concatenate([w[p, pl.ds(q, N, stride=N), :] for p, q in at(i)], axis=1)

    def store_w(i, y):
        for half, (p, q) in enumerate(at(i)):
            w[p, pl.ds(q, N, stride=N), :] = y[:, LANES * half : LANES * (half + 1)]

    def ahead_b(i, x):
        y = down(ahead[...], x)
        return y * jnp.concatenate([factors[pl.ds(pl.multiple_of(q * N, 8), N), :] for _, q in at(i)], axis=1)

    def middle(i):
        now = [i * strip + k for k in range(strip)]
        before = [i * strip - strip + k for k in range(strip)]
        xs, ys = [load_w(q) for q in now], [load_w(q) for q in before]
        xs = [ahead_b(q, x) for q, x in zip(now, xs)]
        ys = [down(back[...], y) for y in ys]
        for q, x in zip(now, xs):
            store_w(q, x)
        for q, y in zip(before, ys):
            store_w(q, y)

    count = N * pairs // 2
    for q, x in [(q, ahead_b(q, load_w(q))) for q in range(strip)]:
        store_w(q, x)
    loop(count // strip, middle, 1)
    for q, y in [(q, down(back[...], load_w(q))) for q in range(count - strip, count)]:
        store_w(q, y)

    total = {}
    for k in range(8):
        where = places_of(blocks_with(k))
        x = jnp.concatenate(
            [
                jnp.concatenate([w[p, pl.ds(line(t, k) + half * N, N), :] for half in range(2)], axis=1)
                for p, t in where
            ],
            axis=0,
        )
        y = along(x, lane_back[k, 0], lane_back[k, 1])
        for i, (p, t) in enumerate(where):
            for half in range(2):
                part = y[N * i : N * (i + 1), LANES * half : LANES * (half + 1)]
                key = (p, 9 * t + 2 * N * k // LANES + half)
                total[key] = total[key] + part if key in total else part
    for (p, tile), value in total.items():
        u[p, :, LANES * tile : LANES * (tile + 1)] = value

    last = pl.ds(LAST, LENGTH - LAST)
    for out, new in list(zip(home_outs, first[0])) + [(visit_out, first[1])]:
        if new:
            for h in range(2):
                out[h, :, last] = jnp.zeros((8, LENGTH - LAST), jnp.float32)

    def flat_back(tiles):
        for fold, at, width in tiles:
            vs = [down(half_back[fold], u[p, :, pl.ds(at, width)]) for p in range(pairs)]
            for h in range(2):
                for i, lanes in enumerate(lanes_of(fold, at, width)):
                    total = visit_out[h, :, lanes] if i == 4 or not first[1] else 0.0
                    other = visit[h, :, lanes]
                    for p in range(pairs):
                        part = vs[p][40 * h + 8 * i : 40 * h + 8 * (i + 1)]
                        before = home_outs[p][h, :, lanes] if i == 4 or not first[0][p] else 0.0
                        home_outs[p][h, :, lanes] = before - part * other
                        total = total - part * homes[p][h, :, lanes]
                    visit_out[h, :, lanes] = total

    flat_back(tiles)


HBM = pl.BlockSpec(memory_space=pl.ANY)
VMEM = pl.BlockSpec(memory_space=pltpu.VMEM)


def places():
    n, g, count = lax.axis_index("band"), lax.axis_index("grid"), lax.axis_size("band")
    core, r = lax.rem(n, 2), lax.rem(n, 4)
    swap = (n, 1 - g)
    x_to = (lax.rem(n + 2, count), 1 - g)
    x_from = (jnp.where(r == 1, n + 1, lax.rem(n + count - 2, count)), 1 - g)
    r_to = (lax.rem(n + count - 1, count), 1 - g)
    y_to, y_from = (lax.rem(n + 1 + 2 * core, count), g), (lax.rem(n + count - 3 + 2 * core, count), g)
    side = (n + 1 - 2 * core, g)
    return g, r, swap, x_to, x_from, r_to, y_to, y_from, side


def greet(senders):
    barrier = pltpu.get_barrier_semaphore()
    for use, device in senders:

        def signal():
            pl.semaphore_signal(barrier, inc=1, device_id=device, device_id_type=MESH)

        signal() if use is None else pl.when(use)(signal)


def blocked(raw, b, out):
    for i in range(4):
        out[:, LINE * i : LINE * i + PLANE] = raw[8 * i : 8 * (i + 1), b, :]
        out[:, LINE * i + PLANE : LINE * (i + 1)] = jnp.zeros((8, LINE - PLANE), jnp.float32)
    end = LAST + PLANE - FOLD
    out[:4, LAST : LAST + FOLD] = raw[32:, b, :FOLD]
    out[:4, LAST + FOLD :] = jnp.zeros((4, LENGTH - LAST - FOLD), jnp.float32)
    out[4:, LAST:end] = raw[32:, b, FOLD:]
    out[4:, end:] = jnp.zeros((4, LENGTH - end), jnp.float32)


def unblocked(part, raw, b):
    for i in range(4):
        raw[8 * i : 8 * (i + 1), b, :] = part(slice(0, 8), slice(LINE * i, LINE * i + PLANE))
    raw[32:, b, :FOLD] = part(slice(0, 4), slice(LAST, LAST + FOLD))
    raw[32:, b, FOLD:] = part(slice(4, 8), slice(LAST, LAST + PLANE - FOLD))


def sender(send, recv):
    index = iter(range(64))

    def make(src, dst, device, into=None):
        i = next(index)
        j = i if into is None else into
        copy = pltpu.make_async_remote_copy(src, dst, send.at[i], recv.at[j], device_id=device, device_id_type=MESH)
        return copy, i

    return make


def exchange_kernel(
    bands, ahead, back, half_ahead, half_back, wide_ahead, wide_back, out,
    flat, outs, lane_ahead, lane_back, factors, u, w, from_s, from_x, from_y, from_r, from_e, raw, send, recv, local,
):
    g, r, swap, x_to, x_from, r_to, y_to, y_from, side = places()
    sends_x, relays = r != 3, r == 2
    f = 1 - g
    pieces = range(len(CHUNKS))
    make = sender(send, recv)

    def cells(c):
        return pl.ds(*CHUNKS[c])

    def many(src, dst, device, into=None):
        made = [
            make(src.at[:, cells(c)], dst.at[:, cells(c)], device, None if into is None else into[c]) for c in pieces
        ]
        return [copy for copy, _ in made], [i for _, i in made]

    load = pltpu.make_async_copy(bands, raw, local.at[0])
    load.start()
    greet([(None, swap), (None, x_from), (None, y_from), (None, side)])
    load.wait()
    for b in range(2):
        blocked(raw, b, flat.at[b, g])
    pl.semaphore_wait(pltpu.get_barrier_semaphore(), 3 + jnp.where(sends_x, 1, 0) + jnp.where(relays, 1, 0))
    e1, _ = many(flat.at[g, g], flat.at[g, g], swap)
    x1, x1_at = make(flat.at[f, g], flat.at[2, g], x_to)
    y1, _ = make(flat.at[f, g], flat.at[4, g], y_to)
    e2, _ = make(flat.at[f, g], flat.at[f, g], swap)
    x2, x2_at = many(flat.at[f, f], flat.at[2, f], x_to)
    y2, _ = many(flat.at[f, f], flat.at[4, f], y_to)
    s1, _ = make(flat.at[2, f], flat.at[3, f], side)
    s2, _ = many(flat.at[2, g], flat.at[3, g], side)
    r1, _ = make(flat.at[4, g], flat.at[2, g], r_to, x1_at)
    r2, _ = many(flat.at[4, f], flat.at[2, f], r_to, x2_at)
    for copy in e1:
        copy.start()

    @pl.when(sends_x)
    def _():
        x1.start()

    y1.start()
    fill_tables(wide_ahead, wide_back, lane_ahead, lane_back, factors)
    for c in pieces:
        e1[c].wait_recv()

        @pl.when(sends_x)
        def _():
            x2[c].start()

        y2[c].start()
    e2.start()

    def pairs(homes, slot, first):
        exchange(
            [flat.at[b] for b in homes], flat.at[slot], [outs.at[b] for b in homes], outs.at[slot], first,
            (ahead, back, half_ahead, half_back), lane_ahead, lane_back, factors, u, w,
        )

    s_back = [many(outs.at[3, h], from_s.at[h], side)[0] for h in (g, f)]
    y_back = [many(outs.at[4, h], from_y.at[h], y_from)[0] for h in (f, g)]
    x_back = [many(outs.at[2, h], from_x.at[h], x_from)[0] for h in (g, f)]
    r_back = [many(outs.at[2, h], from_r.at[h], x_from)[0] for h in (g, f)]
    e1_back, _ = make(outs.at[g, f], from_e.at[g], swap)
    e2_back, _ = many(outs.at[f, f], from_e.at[f], swap)

    y1.wait_recv()

    @pl.when(relays)
    def _():
        r1.start()

    for c in pieces:
        y2[c].wait_recv()

        @pl.when(relays)
        def _():
            r2[c].start()

    outs[4] = jnp.zeros((2, 8, LENGTH), jnp.float32)

    def with_y(i, _):
        @pl.when(i == 1)
        def _():
            e2.wait_recv()

        pairs([lax.rem(f + i, 2)], 4, ((True,), False))
        return 0

    lax.fori_loop(0, 2, with_y, 0)

    @pl.when(r != 2)
    def _():
        for copy in y_back[0] + y_back[1]:
            copy.start()

    x1.wait_recv()
    s1.start()
    for c in pieces:
        x2[c].wait_recv()
        s2[c].start()

    def with_x_and_s(i, _):
        @pl.when(i == 1)
        def _():
            for copy in [s1] + s2:
                copy.wait_recv()

        pairs([0, 1], 2 + i, ((False, False), True))
        return 0

    lax.fori_loop(0, 2, with_x_and_s, 0)
    for copy in s_back[0] + s_back[1]:
        copy.start()
    e1_back.start()
    for k, h in enumerate((g, f)):
        for c in pieces:
            s_back[k][c].wait_recv()
            outs[2, h, :, cells(c)] += from_s[h, :, cells(c)]

            @pl.when(r != 1)
            def _():
                x_back[k][c].start()

            @pl.when(r == 1)
            def _():
                r_back[k][c].start()

    for k, h in enumerate((f, g)):
        for c in pieces:

            @pl.when(relays)
            def _():
                r_back[k][c].wait_recv()
                outs[4, h, :, cells(c)] += from_r[h, :, cells(c)]
                y_back[k][c].start()

            @pl.when(sends_x)
            def _():
                x_back[k][c].wait_recv()
                outs[f, h, :, cells(c)] += from_x[h, :, cells(c)]

            y_back[k][c].wait_recv()
            outs[f, h, :, cells(c)] += from_y[h, :, cells(c)]
            if k == 0:
                e2_back[c].start()
    for copy in [e1_back] + e2_back:
        copy.wait_recv()
    for b in range(2):
        unblocked(lambda rows, lanes: outs[b, g, rows, lanes] + from_e[b, rows, lanes], raw, b)
    store = pltpu.make_async_copy(raw, out, local.at[0])
    store.start()
    store.wait()
    for copy in e1 + [y1, e2] + y2 + [s1] + s2 + s_back[0] + s_back[1] + y_back[0] + y_back[1] + [e1_back] + e2_back:
        copy.wait_send()

    @pl.when(sends_x)
    def _():
        for copy in [x1] + x2:
            copy.wait_send()

    @pl.when(relays)
    def _():
        for copy in [r1] + r2:
            copy.wait_send()

    @pl.when(r != 1)
    def _():
        for copy in x_back[0] + x_back[1]:
            copy.wait_send()

    @pl.when(r == 1)
    def _():
        for copy in r_back[0] + r_back[1]:
            copy.wait_send()


def local(bands):
    band = pltpu.VMEM((2, 8, LENGTH), jnp.float32)
    five = pltpu.VMEM((5, 2, 8, LENGTH), jnp.float32)
    table = pltpu.VMEM((8, 2, 2 * LANES, 2 * LANES), jnp.float32)
    terms = pl.pallas_call(
        exchange_kernel,
        out_shape=jax.ShapeDtypeStruct((HALF, 2, PLANE), jnp.float32),
        in_specs=[HBM] + [VMEM] * 6,
        out_specs=HBM,
        scratch_shapes=[
            five, five, table, table,
            pltpu.VMEM((ROWS, LANES), jnp.float32),
            pltpu.VMEM((2, N, LINE), jnp.float32),
            pltpu.VMEM((2, ROWS, LANES), jnp.float32),
            band, band, band, band, band,
            pltpu.VMEM((HALF, 2, PLANE), jnp.float32),
            pltpu.SemaphoreType.DMA((64,)), pltpu.SemaphoreType.DMA((64,)), pltpu.SemaphoreType.DMA((1,)),
        ],
        compiler_params=pltpu.CompilerParams(collective_id=0, has_side_effects=True, vmem_limit_bytes=63 * 1024 * 1024),
        name="exchange_terms",
    )(bands.transpose(1, 0, 2), *constants())
    return terms.transpose(1, 0, 2)


def solution(mesh):
    return jax.shard_map(
        local,
        mesh=mesh,
        in_specs=(P("band", "grid", None),),
        out_specs=P("band", "grid", None),
        check_vma=False,
    )
```
